128 devices in a mesh: gx: 4 (over x_lo, core), gy: 4 (over y), gz: 8 (over x_hi, z).
Axes of the slice: x: 4 (x_hi: 2, x_lo: 2; x = x_hi * 2 + x_lo), y: 4, z: 4, core: 2. Of those that a mesh axis runs over, the one named last changes fastest.
Arguments:
- inv_factor: bfloat16 [4, 4, 8, 1536, 1536], P('gx', 'gy', 'gz'), as said below
- coupling: bfloat16 [4, 4, 8, 1536, 1536], P('gx', 'gy', 'gz'), may hold values from -0.15625 to 0.15625
- stiff_gg: bfloat16 [4, 4, 8, 1536, 1536], P('gx', 'gy', 'gz'), as said below
- block_order: int32 [4, 4, 8, 12], P('gx', 'gy', 'gz'), may hold values from 0 to 11, each once within a row
Outputs:
- assembled: float32 [4, 4, 8, 1536, 1536], P('gx', 'gy', 'gz')
The draws below stay inside these ranges and needn't reach their ends.
Inputs may be any that keep to these rules, and one draw needn't show every extreme that they name: `block_order`: each subdomain's row is a permutation of 0 to 11. `stiff_gg`: each subdomain's block is symmetric. `inv_factor`: each subdomain's block is lower triangular with a positive diagonal.
All inputs are finite; a program needn't handle non-finite values.
Results may differ from the reference program's by a relative error of at most 0.0016.
Values sent between devices are 32-bit elements; how exact they have to be, the bound alone decides.
No kernel may reach another device: no remote copies, remote signals or barrier semaphores. Data moves between devices by JAX's collectives and lax.ppermute only.
A program may use at most 128 MiB of HBM per device.

```python
import math
import jax
import jax.numpy as jnp
import numpy as np
from jax import lax

NI = 1536
BLK = 128
NBLK = 12
NG = 1536
SUB_X = 4
SUB_Y = 4
SUB_Z = 8


def draw_inv_factor(key, part):
    shape = (SUB_X, SUB_Y, SUB_Z, NI, NI)
    first_key, second_key = jax.random.split(jax.random.fold_in(key, 11))
    entries = jax.random.normal(first_key, shape, jnp.float32)
    lower = jnp.tril(entries, -1) / math.sqrt(NI)
    diagonal = jax.random.uniform(second_key, shape[:-1], jnp.float32, 0.5, 1.5)
    return (lower + diagonal[..., None] * jnp.eye(NI, dtype=jnp.float32)).astype(jnp.bfloat16)


def draw_stiff_gg(key, part):
    shape = (SUB_X, SUB_Y, SUB_Z, NG, NG)
    first_key, second_key = jax.random.split(jax.random.fold_in(key, 23))
    base = jax.random.normal(first_key, shape, jnp.float32)
    symmetric = (base + jnp.swapaxes(base, -1, -2)) / math.sqrt(2.0 * NG)
    diagonal = jax.random.uniform(second_key, shape[:-1], jnp.float32, 2.0, 4.0)
    return (symmetric + diagonal[..., None] * jnp.eye(NG, dtype=jnp.float32)).astype(jnp.bfloat16)


def block_levels(rng, shape, shards, smallest, top_value):
    gain, own = 1.0, jax.random.fold_in(rng, 6)
    for position, parts in shards:
        steps = jnp.exp(jax.random.uniform(jax.random.fold_in(own, position), (parts,), jnp.float32, smallest / len(shards), top_value / len(shards)))
        gain = gain * jnp.repeat(steps, shape[position] // parts).reshape([-1 if axis == position else 1 for axis in range(len(shape))])
    return gain


def bell_draw(rng, shape, scale, limit, cuts=(), kind=jnp.bfloat16):
    values = jax.random.normal(rng, shape, jnp.float32) * scale
    if len(cuts) > 0:
        values = block_levels(rng, shape, cuts, -0.22, 0.18) * values
    return jnp.clip(values, min=-limit, max=limit).astype(kind)


def setup_inputs(seed: int = 0) -> dict:
    keys = jax.random.split(jax.random.key(seed), 5)
    return {
        "inv_factor": draw_inv_factor(jax.random.fold_in(keys[4], 71), 0),
        "coupling": bell_draw(keys[1], (SUB_X, SUB_Y, SUB_Z, NI, NG), NI ** -0.5, 0.15625, ((0, 4), (1, 4), (2, 8))),
        "stiff_gg": draw_stiff_gg(jax.random.fold_in(keys[4], 71), 0),
        "block_order": jax.vmap(lambda own: jax.random.permutation(own, NBLK))(jax.random.split(keys[3], SUB_X * SUB_Y * SUB_Z)).reshape((SUB_X, SUB_Y, SUB_Z, NBLK)).astype(jnp.int32),
    }


west_blocks = (0,)
east_blocks = (1,)
south_blocks = (2, 8, 10)
north_blocks = (3, 9, 11)
bottom_blocks = (4, 5, 8, 9)
top_blocks = (6, 7, 10, 11)


def local_tile(operands):
    inverse, coupled, stiffness = operands
    weighted = jnp.dot(inverse, coupled, preferred_element_type=jnp.float32).astype(jnp.bfloat16)
    product = jnp.dot(weighted.T, weighted, preferred_element_type=jnp.float32)
    return stiffness.astype(jnp.float32) - product


def reorder(matrix, ranking):
    return matrix[ranking][:, ranking]


def shifted(values, axis, direction):
    extent = values.shape[axis]
    zeros_edge = jnp.zeros_like(lax.slice_in_dim(values, 0, 1, axis=axis))
    if direction > 0:
        return jnp.concatenate([zeros_edge, lax.slice_in_dim(values, 0, extent - 1, axis=axis)], axis)
    return jnp.concatenate([lax.slice_in_dim(values, 1, extent, axis=axis), zeros_edge], axis)


def section_sum(grid, axis, lower_list, upper_list):
    lower_idx = np.array(lower_list, dtype=np.int32)
    upper_idx = np.array(upper_list, dtype=np.int32)
    lower_piece = grid[:, :, :, lower_idx][:, :, :, :, lower_idx]
    upper_piece = grid[:, :, :, upper_idx][:, :, :, :, upper_idx]
    from_lower = shifted(upper_piece, axis, 1)
    from_upper = shifted(lower_piece, axis, -1)
    grid = grid.at[:, :, :, lower_idx[:, None], lower_idx[None, :]].add(from_lower)
    grid = grid.at[:, :, :, upper_idx[:, None], upper_idx[None, :]].add(from_upper)
    return grid


def reference(inv_factor, coupling, stiff_gg, block_order):
    total = SUB_X * SUB_Y * SUB_Z
    tiles = lax.map(local_tile, (inv_factor.reshape(total, NI, NI), coupling.reshape(total, NI, NG), stiff_gg.reshape(total, NG, NG)))
    blocked = tiles.reshape(total, NBLK, BLK, NBLK, BLK).transpose(0, 1, 3, 2, 4)
    ranks = block_order.reshape(total, NBLK).astype(jnp.int32)
    canonical = jax.vmap(reorder)(blocked, ranks)
    grid = canonical.reshape(SUB_X, SUB_Y, SUB_Z, NBLK, NBLK, BLK, BLK)
    grid = section_sum(grid, 0, west_blocks, east_blocks)
    grid = section_sum(grid, 1, south_blocks, north_blocks)
    grid = section_sum(grid, 2, bottom_blocks, top_blocks)
    inverse_rank = jnp.argsort(ranks, axis=1).astype(jnp.int32)
    own = jax.vmap(reorder)(grid.reshape(total, NBLK, NBLK, BLK, BLK), inverse_rank)
    return own.transpose(0, 1, 3, 2, 4).reshape(SUB_X, SUB_Y, SUB_Z, NG, NG)
```

```python
import functools

import jax
import jax.numpy as jnp
from jax import lax
from jax.experimental import pallas as pl
from jax.experimental.pallas import tpu as pltpu
from jax.sharding import PartitionSpec as P

BLK = 128
NBLK = 12
PAN = 256

FIRST = (4, 5, 8, 9, 6, 7, 10, 11)
SECOND = (2, 3, 0, 1)
PAIRS = {"A": (4, 5), "B": (8, 9), "C": (6, 7), "D": (10, 11), "E": (2, 3), "F": (0, 1)}
BOTTOM = (4, 5, 8, 9)
TOP = (6, 7, 10, 11)
SOUTH = (2, 8, 10)
NORTH = (3, 9, 11)
REST = ("AC", "AD", "BC", "EA", "EC", "FA", "FB", "FC", "FD", "FE")


def upper(listed):
    return [(k, l) for i, k in enumerate(listed) for l in listed[i:]]


Z_LOW, Z_HIGH = upper(BOTTOM), upper(TOP)
Y_LOW, Y_HIGH = upper(SOUTH), upper(NORTH)
MIXED = ("EE", "EB", "ED", "BD", "FF")


def block_start(order, k):
    return pl.multiple_of(order[k] * BLK, BLK)


def stiff_copy(order, stiff, buf, sem, slot, k, l):
    return pltpu.make_async_copy(
        stiff.at[pl.ds(block_start(order, k), BLK), pl.ds(block_start(order, l), BLK)],
        buf.at[slot],
        sem,
    )


def column_copies(order, coupling, buf, sems, listed):
    copies = []
    for pan in range(buf.shape[0] // PAN):
        rows = pl.ds(pan * PAN, PAN)
        copies.append(
            [
                pltpu.make_async_copy(
                    coupling.at[rows, pl.ds(block_start(order, k), BLK)],
                    buf.at[rows, pl.ds(at * BLK, BLK)],
                    sems.at[pan],
                )
                for at, k in enumerate(listed)
            ]
        )
    return copies


def factor_copies(inverse, buf, sems):
    return [
        pltpu.make_async_copy(
            inverse.at[pl.ds(pan * PAN, PAN), pl.ds(0, (pan + 1) * PAN)],
            buf.at[pl.ds(pan * PAN, PAN), pl.ds(0, (pan + 1) * PAN)],
            sems.at[pan],
        )
        for pan in range(inverse.shape[0] // PAN)
    ]


def weigh(inverse, coupled, pan):
    depth = (pan + 1) * PAN
    return jnp.dot(
        inverse[pan * PAN : depth, :depth], coupled[:depth, :], preferred_element_type=jnp.float32
    ).astype(jnp.bfloat16)


def gram(left, right):
    return lax.dot_general(left, right, (((0,), (0,)), ((), ())), preferred_element_type=jnp.float32)


def first_kernel(order, inverse, coupling, stiff, zd, zu, w1, lbuf, cbuf, sbuf, lsem, csem, ssem):
    lcopies = factor_copies(inverse, lbuf, lsem)
    ccopies = column_copies(order, coupling, cbuf, csem, FIRST)
    for lcopy, group in zip(lcopies, ccopies):
        lcopy.start()
        for copy in group:
            copy.start()
    blocks = Z_LOW + Z_HIGH
    scopies = [stiff_copy(order, stiff, sbuf, ssem, i, k, l) for i, (k, l) in enumerate(blocks)]
    for copy in scopies:
        copy.start()
    for pan, (lcopy, group) in enumerate(zip(lcopies, ccopies)):
        lcopy.wait()
        for copy in group:
            copy.wait()
        w1[pan * PAN : (pan + 1) * PAN, :] = weigh(lbuf, cbuf, pan)
    for copy in scopies:
        copy.wait()
    for base, out, listed, half in ((0, zd, BOTTOM, 0), (10, zu, TOP, 512)):
        pairs = upper(listed)
        first = gram(w1[:, half : half + 256], w1[:, half : half + 512])
        second = gram(w1[:, half + 256 : half + 512], w1[:, half + 256 : half + 512])
        for n, (k, l) in enumerate(pairs):
            i, j = listed.index(k), listed.index(l)
            source, row, col = (first, i, j) if i < 2 else (second, i - 2, j - 2)
            out[n] = sbuf[base + n].astype(jnp.float32) - source[
                row * BLK : (row + 1) * BLK, col * BLK : (col + 1) * BLK
            ]


def second_kernel(order, inverse, coupling, stiff, w1, zd, zu, yd, yu, xd, xu, w2, keep, lbuf, cbuf, sbuf, lsem, csem, ssem):
    lcopies = factor_copies(inverse, lbuf, lsem)
    ccopies = column_copies(order, coupling, cbuf, csem, SECOND)
    for lcopy, group in zip(lcopies, ccopies):
        lcopy.start()
        for copy in group:
            copy.start()
    blocks = [(k, l) for name in MIXED for k, l in cells(name)]
    scopies = [stiff_copy(order, stiff, sbuf, ssem, i, k, l) for i, (k, l) in enumerate(blocks)]
    for copy in scopies:
        copy.start()
    for pan, (lcopy, group) in enumerate(zip(lcopies, ccopies)):
        lcopy.wait()
        for copy in group:
            copy.wait()
        w2[pan * PAN : (pan + 1) * PAN, :] = weigh(lbuf, cbuf, pan)
    for copy in scopies:
        copy.wait()
    yd[Y_LOW.index((8, 8))] = zd[Z_LOW.index((8, 8))]
    yd[Y_LOW.index((10, 10))] = zu[Z_HIGH.index((10, 10))]
    yu[Y_HIGH.index((9, 9))] = zd[Z_LOW.index((9, 9))]
    yu[Y_HIGH.index((11, 11))] = zu[Z_HIGH.index((11, 11))]
    targets = {}
    for n, pair in enumerate(Y_LOW):
        targets[pair] = (yd, n)
    for n, pair in enumerate(Y_HIGH):
        targets[pair] = (yu, n)
    targets[(0, 0)], targets[(1, 1)] = (xd, 0), (xu, 0)
    at = kept = 0
    for name in MIXED:
        result = gram(part(name[0], w1, w2), part(name[1], w1, w2))
        rows, cols = PAIRS[name[0]], PAIRS[name[1]]
        for k, l in cells(name):
            row, col = rows.index(k), cols.index(l)
            value = sbuf[at].astype(jnp.float32) - result[
                row * BLK : (row + 1) * BLK, col * BLK : (col + 1) * BLK
            ]
            at += 1
            if (k, l) in targets:
                out, slot = targets[(k, l)]
                out[slot] = value
            else:
                keep[kept] = value
                kept += 1


def cells(name):
    rows, cols = PAIRS[name[0]], PAIRS[name[1]]
    return [(k, l) for k in rows for l in cols if name[0] != name[1] or k <= l]


def part(letter, w1, w2):
    if letter in "ABCD":
        at = "ABCD".index(letter) * 256
        return w1[:, at : at + 256]
    at = "EF".index(letter) * 256
    return w2[:, at : at + 256]


SHARED = set(Z_LOW + Z_HIGH + Y_LOW + Y_HIGH + [(0, 0), (1, 1)])
KEPT = [cell for name in MIXED for cell in cells(name) if cell not in SHARED]


def put(order, out, stage, sem, slot, k, l):
    copy = pltpu.make_async_copy(
        stage.at[slot],
        out.at[pl.ds(block_start(order, k), BLK), pl.ds(block_start(order, l), BLK)],
        sem,
    )
    copy.start()
    return copy


def rest_kernel(order, stiff, w1, w2, keep, out, sbuf, stage, ssem, osem):
    blocks = [(k, l) for name in REST for k, l in cells(name)]
    scopies = [stiff_copy(order, stiff, sbuf, ssem, i, k, l) for i, (k, l) in enumerate(blocks)]
    for copy in scopies:
        copy.start()
    copies = []

    def emit(k, l, value):
        slot = len(copies)
        stage[slot] = value
        copies.append(put(order, out, stage, osem, slot, k, l))
        stage[slot + 1] = value.T
        copies.append(put(order, out, stage, osem, slot + 1, l, k))

    for n, (k, l) in enumerate(KEPT):
        emit(k, l, keep[n])
    for copy in scopies:
        copy.wait()
    at = 0
    for name in REST:
        result = gram(part(name[0], w1, w2), part(name[1], w1, w2))
        rows, cols = PAIRS[name[0]], PAIRS[name[1]]
        for k, l in cells(name):
            row, col = rows.index(k), cols.index(l)
            emit(
                k,
                l,
                sbuf[at].astype(jnp.float32)
                - result[row * BLK : (row + 1) * BLK, col * BLK : (col + 1) * BLK],
            )
            at += 1
    for copy in copies:
        copy.wait()


def last_kernel(order, zd, zu, yd, yu, xd, xu, fzl, fzh, fyl, fyh, fxl, fxh, cll, clh, chl, chh, before, out, stage, osem):
    copies = []

    def emit(k, l, value):
        slot = len(copies)
        stage[slot] = value
        copies.append(put(order, out, stage, osem, slot, k, l))
        if k != l:
            stage[slot + 1] = value.T
            copies.append(put(order, out, stage, osem, slot + 1, l, k))

    edges = {8: (fyl, Y_HIGH.index((9, 9)), cll), 9: (fyh, Y_LOW.index((8, 8)), chl)}
    edges[10] = (fyl, Y_HIGH.index((11, 11)), clh)
    edges[11] = (fyh, Y_LOW.index((10, 10)), chh)
    emit(0, 0, xd[0] + fxl[0])
    emit(1, 1, xu[0] + fxh[0])
    for pairs, own, other in ((Y_LOW, yd, fyl), (Y_HIGH, yu, fyh)):
        for n, (k, l) in enumerate(pairs):
            if k != l or k in (2, 3):
                emit(k, l, own[n] + other[n])
    for pairs, own, other in ((Z_LOW, zd, fzl), (Z_HIGH, zu, fzh)):
        for n, (k, l) in enumerate(pairs):
            value = own[n] + other[n]
            if k == l and k in edges:
                across, slot, corner = edges[k]
                value = value + across[slot] + corner[0]
            emit(k, l, value)
    for copy in copies:
        copy.wait()


def shifts(axis):
    size = lax.axis_size(axis)
    return [(i, i + 1) for i in range(size - 1)]


def swap(pairs):
    return [(j, i) for i, j in pairs]


HBM = pl.BlockSpec(memory_space=pltpu.HBM)
VMEM = pl.BlockSpec(memory_space=pltpu.VMEM)
SMEM = pl.BlockSpec(memory_space=pltpu.SMEM)
MB = 1024 * 1024


def shape(*dims, dtype=jnp.float32):
    return jax.ShapeDtypeStruct(dims, dtype)


def params(limit):
    return pltpu.CompilerParams(vmem_limit_bytes=limit * MB)


def shards(inv_factor, coupling, stiff_gg, block_order):
    rows = inv_factor.shape[3]
    order = block_order.reshape(NBLK)
    inverse = inv_factor.reshape(rows, rows)
    coupled = coupling.reshape(rows, NBLK * BLK)
    stiff = stiff_gg.reshape(NBLK * BLK, NBLK * BLK)
    panels = rows // PAN
    dma = pltpu.SemaphoreType.DMA
    zd, zu, w1 = pl.pallas_call(
        first_kernel,
        out_shape=(shape(10, BLK, BLK), shape(10, BLK, BLK), shape(rows, 1024, dtype=jnp.bfloat16)),
        in_specs=[SMEM, HBM, HBM, HBM],
        out_specs=(VMEM, VMEM, VMEM),
        scratch_shapes=[
            pltpu.VMEM((rows, rows), jnp.bfloat16),
            pltpu.VMEM((rows, 1024), jnp.bfloat16),
            pltpu.VMEM((20, BLK, BLK), jnp.bfloat16),
            dma((panels,)),
            dma((panels,)),
            dma,
        ],
        compiler_params=params(30),
        cost_estimate=pl.CostEstimate(flops=6 * 10**9, bytes_accessed=8 * 10**6, transcendentals=0),
        name="first",
    )(order, inverse, coupled, stiff)
    up, down = shifts("gz"), swap(shifts("gz"))
    fzl = lax.ppermute(zu, "gz", up)
    fzh = lax.ppermute(zd, "gz", down)
    mixed = sum(len(cells(name)) for name in MIXED)
    yd, yu, xd, xu, w2, keep = pl.pallas_call(
        second_kernel,
        out_shape=(
            shape(6, BLK, BLK),
            shape(6, BLK, BLK),
            shape(1, BLK, BLK),
            shape(1, BLK, BLK),
            shape(rows, 512, dtype=jnp.bfloat16),
            shape(len(KEPT), BLK, BLK),
        ),
        in_specs=[SMEM, HBM, HBM, HBM, VMEM, VMEM, VMEM],
        out_specs=(VMEM,) * 6,
        scratch_shapes=[
            pltpu.VMEM((rows, rows), jnp.bfloat16),
            pltpu.VMEM((rows, 512), jnp.bfloat16),
            pltpu.VMEM((mixed, BLK, BLK), jnp.bfloat16),
            dma((panels,)),
            dma((panels,)),
            dma,
        ],
        compiler_params=params(30),
        cost_estimate=pl.CostEstimate(flops=4 * 10**9, bytes_accessed=8 * 10**6, transcendentals=0),
        name="second",
    )(order, inverse, coupled, stiff, w1, zd, zu)
    sy, ny = shifts("gy"), swap(shifts("gy"))
    fyl = lax.ppermute(yu, "gy", sy)
    fyh = lax.ppermute(yd, "gy", ny)
    size = lax.axis_size("gz")

    def corner(block, ypairs, zpairs):
        pairs = [(a * size + c, b * size + d) for a, b in ypairs for c, d in zpairs]
        return lax.ppermute(block, ("gy", "gz"), pairs)

    cll = corner(zu[9:10], sy, up)
    clh = corner(zd[9:10], sy, down)
    chl = corner(zu[7:8], ny, up)
    chh = corner(zd[7:8], ny, down)
    fxl = lax.ppermute(xu, "gx", shifts("gx"))
    fxh = lax.ppermute(xd, "gx", swap(shifts("gx")))
    out = pl.pallas_call(
        rest_kernel,
        out_shape=shape(NBLK * BLK, NBLK * BLK),
        in_specs=[SMEM, HBM, VMEM, VMEM, VMEM],
        out_specs=HBM,
        scratch_shapes=[
            pltpu.VMEM((40, BLK, BLK), jnp.bfloat16),
            pltpu.VMEM((96, BLK, BLK), jnp.float32),
            dma,
            dma,
        ],
        compiler_params=params(30),
        cost_estimate=pl.CostEstimate(flops=2 * 10**9, bytes_accessed=8 * 10**6, transcendentals=0),
        name="rest",
    )(order, stiff, w1, w2, keep)
    out = pl.pallas_call(
        last_kernel,
        out_shape=shape(NBLK * BLK, NBLK * BLK),
        in_specs=[SMEM] + [VMEM] * 16 + [HBM],
        out_specs=HBM,
        scratch_shapes=[pltpu.VMEM((48, BLK, BLK), jnp.float32), dma],
        input_output_aliases={17: 0},
        compiler_params=params(20),
        cost_estimate=pl.CostEstimate(flops=10**6, bytes_accessed=8 * 10**6, transcendentals=0),
        name="last",
    )(order, zd, zu, yd, yu, xd, xu, fzl, fzh, fyl, fyh, fxl, fxh, cll, clh, chl, chh, out)
    return out.reshape(1, 1, 1, NBLK * BLK, NBLK * BLK)


def solution(mesh):
    return jax.shard_map(
        shards,
        mesh=mesh,
        in_specs=(
            P("gx", "gy", "gz", None, None),
            P("gx", "gy", "gz", None, None),
            P("gx", "gy", "gz", None, None),
            P("gx", "gy", "gz", None),
        ),
        out_specs=P("gx", "gy", "gz", None, None),
        check_vma=False,
    )
```

```python
import jax
import jax.numpy as jnp
from jax import lax
from jax.experimental import pallas as pl
from jax.experimental.pallas import tpu as pltpu
from jax.sharding import PartitionSpec as P

BLK = 128
NBLK = 12
PAN = 256

PAIRS = {"A": (4, 5), "B": (8, 9), "C": (6, 7), "D": (10, 11), "E": (2, 3), "F": (0, 1)}
COLUMNS = (8, 9, 10, 11, 4, 5, 6, 7, 2, 3, 0, 1)
Z_HIGH, Z_LOW = ((6, 7), (6, 10), (6, 11), (7, 10), (7, 11), (10, 11)), ((4, 5), (4, 8), (4, 9), (5, 8), (5, 9), (8, 9))
Z_HIGH_PACK, Z_LOW_PACK = ((6, 7), (11, 10)), ((4, 5), (8, 9))
Y_HIGH, Y_LOW = ((3, 3), (3, 9), (3, 11), (9, 11)), ((2, 2), (2, 8), (2, 10), (8, 10))
KEPT = ((2, 3), (2, 9), (3, 8), (2, 11), (3, 10), (8, 11), (9, 10), (0, 1))
FACES = 8 * BLK
MESSAGE = FACES + 8


def position(order, k):
    if k < 2:
        at = k ^ (lax.axis_index("gx") % 2)
    elif k < 4:
        at = 2 + ((k - 2) ^ (lax.axis_index("gy") % 2))
    elif k < 8:
        at = 4 + ((k - 4) ^ (2 * (lax.axis_index("gz") % 2)))
    else:
        at = 8 + ((k - 8) ^ (lax.axis_index("gy") % 2 + 2 * (lax.axis_index("gz") % 2)))
    return pl.multiple_of(order[at] * BLK, BLK)


def positions(order):
    return [position(order, k) for k in range(NBLK)]


def fetch_order(order, osmem, sem):
    copy = pltpu.make_async_copy(order, osmem, sem)
    copy.start()
    return copy


def stiff_copies(at, stiff, buf, sem, blocks):
    copies = [
        pltpu.make_async_copy(
            stiff.at[pl.ds(at[k], BLK), pl.ds(at[l], BLK)], buf.at[pl.ds(n * BLK, BLK), :], sem
        )
        for n, (k, l) in enumerate(blocks)
    ]
    for copy in copies:
        copy.start()
    return copies


def weigh(lbuf, cbuf, columns, pan):
    depth = (pan + 1) * PAN
    return jnp.dot(
        lbuf[pan * PAN : depth, :depth], cbuf[:depth, columns], preferred_element_type=jnp.float32
    ).astype(jnp.bfloat16)


def gram(left, right):
    return lax.dot_general(left, right, (((0,), (0,)), ((), ())), preferred_element_type=jnp.float32)


def rows_ge():
    r = lax.broadcasted_iota(jnp.int32, (BLK, BLK), 0)
    c = lax.broadcasted_iota(jnp.int32, (BLK, BLK), 1)
    return r, c


def pack(first, second):
    r, c = rows_ge()
    return jnp.where(r <= c, first, second), jnp.sum(jnp.where(r == c, second, 0.0), axis=0, keepdims=True)


def unpack(tile, diagonal):
    r, c = rows_ge()
    turned = tile.T
    first = jnp.where(r <= c, tile, turned)
    return first, jnp.where(r > c, tile, jnp.where(r < c, turned, diagonal))


def two_rows(first, second):
    row = lax.broadcasted_iota(jnp.int32, (8, BLK), 0)
    return jnp.where(row == 0, first, jnp.where(row == 1, second, 0.0))


def piece(result, i, j):
    return result[i * BLK : (i + 1) * BLK, j * BLK : (j + 1) * BLK]


def slot(n):
    return slice(n * BLK, (n + 1) * BLK)


EDGE_BLOCKS = ((8, 8), (8, 9), (9, 9), (10, 10), (10, 11), (11, 11))


def edge_kernel(order, inverse, coupling, stiff, lbuf, cbuf, wbd, yda, ydb, zpart, osmem, sbuf, osem, lsem, csem, rsem, ssem):
    fetch = fetch_order(order, osmem, osem)
    panels = lbuf.shape[0] // PAN
    lcopies = [
        pltpu.make_async_copy(
            inverse.at[pl.ds(pan * PAN, PAN), pl.ds(0, (pan + 1) * PAN)],
            lbuf.at[pl.ds(pan * PAN, PAN), pl.ds(0, (pan + 1) * PAN)],
            lsem.at[pan],
        )
        for pan in range(panels)
    ]
    for copy in lcopies[:2]:
        copy.start()
    fetch.wait()
    at = positions(osmem)
    ccopies = []
    for pan in range(panels):
        rows = pl.ds(pan * PAN, PAN)
        group = [
            pltpu.make_async_copy(
                coupling.at[rows, pl.ds(at[k], BLK)], cbuf.at[rows, pl.ds(n * BLK, BLK)], csem.at[pan]
            )
            for n, k in enumerate(COLUMNS[:4])
        ]
        ccopies.append(group)
        if pan >= 2:
            lcopies[pan].start()
        for copy in group:
            copy.start()
    scopies = stiff_copies(at, stiff, sbuf, ssem, EDGE_BLOCKS)
    later = [
        pltpu.make_async_copy(
            coupling.at[:, pl.ds(at[k], BLK)], cbuf.at[:, pl.ds((n + 4) * BLK, BLK)], rsem
        )
        for n, k in enumerate(COLUMNS[4:])
    ]
    for copy in later:
        copy.start()
    for pan in range(panels):
        lcopies[pan].wait()
        for copy in ccopies[pan]:
            copy.wait()
        wbd[pan * PAN : (pan + 1) * PAN, :] = weigh(lbuf, cbuf, slice(0, 512), pan)
    for copy in scopies:
        copy.wait()
    full = []
    for n in range(2):
        half = wbd[:, n * 256 : (n + 1) * 256]
        result = gram(half, half)
        for m, (i, j) in enumerate(((0, 0), (0, 1), (1, 1))):
            full.append(sbuf[slot(n * 3 + m)].astype(jnp.float32) - piece(result, i, j))
    b8, b89, b9, b10, b1011, b11 = full
    ydb[:BLK], row = pack(b8, b10)
    ydb[BLK:] = two_rows(row, 0.0)
    yda[:BLK], row = pack(b11, b9)
    yda[BLK:] = two_rows(row, 0.0)
    zpart[slot(0)] = b89
    zpart[slot(1)] = b1011
    zpart[slot(2)], low = pack(b8, b9)
    zpart[slot(3)], high = pack(b11, b10)
    zpart[4 * BLK :] = two_rows(low, high)
    for copy in later:
        copy.wait()


FACE_BLOCKS = ((4, 4), (4, 5), (5, 5), (4, 8), (4, 9), (5, 8), (5, 9), (6, 6), (6, 7), (7, 7), (6, 10), (6, 11), (7, 10), (7, 11))


def face_kernel(order, stiff, lbuf, cbuf, wbd, zpart, wac, za, zb, osmem, sbuf, osem, ssem):
    fetch_order(order, osmem, osem).wait()
    at = positions(osmem)
    scopies = stiff_copies(at, stiff, sbuf, ssem, FACE_BLOCKS)
    for pan in range(lbuf.shape[0] // PAN):
        wac[pan * PAN : (pan + 1) * PAN, :] = weigh(lbuf, cbuf, slice(512, 1024), pan)
    for copy in scopies:
        copy.wait()
    for n, (out, part) in enumerate(((zb, 0), (za, 1))):
        own = wac[:, n * 256 : (n + 1) * 256]
        inner = gram(own, own)
        outer = gram(own, wbd[:, n * 256 : (n + 1) * 256])
        base = n * 7

        def value(m, result, i, j):
            return sbuf[slot(base + m)].astype(jnp.float32) - piece(result, i, j)

        out[slot(6)], row = pack(value(0, inner, 0, 0), value(2, inner, 1, 1))
        out[slot(0)] = value(1, inner, 0, 1)
        for m, (i, j) in enumerate(((0, 0), (0, 1), (1, 0), (1, 1))):
            out[slot(1 + m)] = value(3 + m, outer, i, j)
        out[slot(5)] = zpart[slot(part)]
        out[slot(7)] = zpart[slot(2 + part)]
        out[FACES:] = two_rows(row, zpart[4 * BLK + part : 4 * BLK + part + 1])


def join_kernel(za, zb, fya, fyb, za_out, zb_out):
    del za, zb
    r, c = rows_ge()
    above = r <= c
    row = lax.broadcasted_iota(jnp.int32, (8, BLK), 0) == 1
    za_out[slot(7)] = za_out[slot(7)] + jnp.where(above, fya[:BLK], fyb[:BLK])
    za_out[FACES:] = za_out[FACES:] + jnp.where(row, fyb[BLK : BLK + 1], 0.0)
    zb_out[slot(7)] = zb_out[slot(7)] + jnp.where(above, fyb[:BLK], fya[:BLK])
    zb_out[FACES:] = zb_out[FACES:] + jnp.where(row, fya[BLK : BLK + 1], 0.0)


SIDE_BLOCKS = tuple((k, l) for k in (2, 3) for l in (2, 3, 8, 9, 10, 11) if k <= l) + ((8, 10), (8, 11), (9, 10), (9, 11), (0, 0), (0, 1), (1, 1))


def side_kernel(order, stiff, lbuf, cbuf, wbd, after, wef, yea, yeb, xa, xb, keep, osmem, sbuf, osem, ssem):
    del after
    fetch_order(order, osmem, osem).wait()
    at = positions(osmem)
    scopies = stiff_copies(at, stiff, sbuf, ssem, SIDE_BLOCKS)
    for pan in range(lbuf.shape[0] // PAN):
        wef[pan * PAN : (pan + 1) * PAN, :] = weigh(lbuf, cbuf, slice(1024, 1536), pan)
    for copy in scopies:
        copy.wait()
    e, f = wef[:, :256], wef[:, 256:]
    targets = {pair: (yea, n) for n, pair in enumerate(Y_HIGH)} | {pair: (yeb, n) for n, pair in enumerate(Y_LOW)}
    targets |= {pair: (keep, n) for n, pair in enumerate(KEPT)} | {(1, 1): (xa, 0), (0, 0): (xb, 0)}

    def emit(result, rows, cols):
        for i, k in enumerate(rows):
            for j, l in enumerate(cols):
                if k <= l:
                    out, n = targets[(k, l)]
                    m = SIDE_BLOCKS.index((k, l))
                    out[slot(n)] = sbuf[slot(m)].astype(jnp.float32) - piece(result, i, j)

    emit(gram(e, e), (2, 3), (2, 3))
    emit(gram(e, wbd[...]), (2, 3), (8, 9, 10, 11))
    emit(gram(wbd[:, :256], wbd[:, 256:]), (8, 9), (10, 11))
    emit(gram(f, f), (0, 1), (0, 1))


REST = (
    ("F", (("bd", (8, 9, 10, 11)), ("ac", (4, 5, 6, 7)), ("e", (2, 3)))),
    ("E", (("ac", (4, 5, 6, 7)),)),
    ("A", (("c", (6, 7)), ("d", (10, 11)))),
    ("C", (("b", (8, 9)),)),
)
REST_BLOCKS = tuple((k, l) for left, rights in REST for _, cols in rights for k in PAIRS[left] for l in cols)


def put(at, out, stage, sem, n, k, l):
    copy = pltpu.make_async_copy(
        stage.at[pl.ds(n * BLK, BLK), :], out.at[pl.ds(at[k], BLK), pl.ds(at[l], BLK)], sem
    )
    copy.start()
    return copy


def rest_kernel(order, stiff, wbd, wac, wef, keep, out, osmem, sbuf, turned, stage, osem, ssem, wsem):
    fetch_order(order, osmem, osem).wait()
    at = positions(osmem)
    scopies = stiff_copies(at, stiff, sbuf, ssem, REST_BLOCKS)
    copies = []

    def emit(k, l, value):
        n = len(copies)
        stage[slot(n)] = value
        copies.append(put(at, out, stage, wsem, n, k, l))
        stage[slot(n + 1)] = value.T
        copies.append(put(at, out, stage, wsem, n + 1, l, k))

    whole = {"ac": (wac, 0, 512), "bd": (wbd, 0, 512), "e": (wef, 0, 256), "f": (wef, 256, 512), "a": (wac, 0, 256)}
    whole |= {"c": (wac, 256, 512), "b": (wbd, 0, 256), "d": (wbd, 256, 512)}
    for n, (k, l) in enumerate(KEPT):
        emit(k, l, keep[slot(n)])
    for copy in scopies:
        copy.wait()
    m = 0
    for left, rights in REST:
        ref, lo, hi = whole[left.lower()]
        turned[...] = ref[:, lo:hi].T
        for name, cols in rights:
            ref, lo, hi = whole[name]
            result = jnp.dot(turned[...], ref[:, lo:hi], preferred_element_type=jnp.float32)
            for i, k in enumerate(PAIRS[left]):
                for j, l in enumerate(cols):
                    emit(k, l, sbuf[slot(m)].astype(jnp.float32) - piece(result, i, j))
                    m += 1
    for copy in copies:
        copy.wait()


def last_kernel(order, za, zb, fza, fzb, yea, yeb, fyea, fyeb, xa, xb, fxa, fxb, before, out, osmem, stage, osem, wsem):
    del before
    fetch_order(order, osmem, osem).wait()
    at = positions(osmem)
    copies = []

    def emit(k, l, value):
        n = len(copies)
        stage[slot(n)] = value
        copies.append(put(at, out, stage, wsem, n, k, l))
        if k != l:
            stage[slot(n + 1)] = value.T
            copies.append(put(at, out, stage, wsem, n + 1, l, k))

    emit(0, 0, xb[...] + fxb[...])
    emit(1, 1, xa[...] + fxa[...])
    for pairs, own, other in ((Y_HIGH, yea, fyea), (Y_LOW, yeb, fyeb)):
        for n, (k, l) in enumerate(pairs):
            emit(k, l, own[slot(n)] + other[slot(n)])
    for pairs, packs, own, other in ((Z_LOW, Z_LOW_PACK, zb, fzb), (Z_HIGH, Z_HIGH_PACK, za, fza)):
        for n, (k, l) in enumerate(pairs):
            emit(k, l, own[slot(n)] + other[slot(n)])
        for n, (k, l) in enumerate(packs):
            row = slice(FACES + n, FACES + n + 1)
            first, second = unpack(own[slot(6 + n)] + other[slot(6 + n)], own[row] + other[row])
            emit(k, k, first)
            emit(l, l, second)
    for copy in copies:
        copy.wait()


def exchange(value, axis, start):
    size = lax.axis_size(axis)
    pairs = [(i, i + 1) for i in range(start, size - 1, 2)]
    return lax.ppermute(value, axis, pairs + [(j, i) for i, j in pairs])


HBM = pl.BlockSpec(memory_space=pltpu.HBM)
VMEM = pl.BlockSpec(memory_space=pltpu.VMEM)
DMA = pltpu.SemaphoreType.DMA


def shape(*dims, dtype=jnp.float32):
    return jax.ShapeDtypeStruct(dims, dtype)


def params(mib):
    return pltpu.CompilerParams(vmem_limit_bytes=mib * 1024 * 1024)


def cost(gigaflops, megabytes):
    return pl.CostEstimate(
        flops=int(gigaflops * 1e9), bytes_accessed=int(megabytes * 1e6), transcendentals=0
    )


def in_hbm(value):
    return pltpu.with_memory_space_constraint(value, pltpu.HBM)


def shards(inv_factor, coupling, stiff_gg, block_order):
    rows = inv_factor.shape[3]
    size = NBLK * BLK
    half = jnp.bfloat16
    order = in_hbm(block_order.reshape(NBLK))
    inverse = in_hbm(inv_factor.reshape(rows, rows))
    coupled = in_hbm(coupling.reshape(rows, size))
    stiff = in_hbm(stiff_gg.reshape(size, size))
    panels = rows // PAN
    osmem = pltpu.SMEM((NBLK,), jnp.int32)

    def stiff_scratch(blocks):
        return pltpu.VMEM((len(blocks) * BLK, BLK), half)

    lbuf, cbuf, wbd, yda, ydb, zpart = pl.pallas_call(
        edge_kernel,
        out_shape=(
            shape(rows, rows, dtype=half),
            shape(rows, size, dtype=half),
            shape(rows, 512, dtype=half),
            shape(BLK + 8, BLK),
            shape(BLK + 8, BLK),
            shape(4 * BLK + 8, BLK),
        ),
        in_specs=[HBM] * 4,
        out_specs=(VMEM,) * 6,
        scratch_shapes=[osmem, stiff_scratch(EDGE_BLOCKS), DMA, DMA((panels,)), DMA((panels,)), DMA, DMA],
        compiler_params=params(12),
        cost_estimate=cost(3, 8),
        name="edges",
    )(order, inverse, coupled, stiff)
    fya = exchange(yda, "gy", 0)
    fyb = exchange(ydb, "gy", 1)
    wac, za, zb = pl.pallas_call(
        face_kernel,
        out_shape=(shape(rows, 512, dtype=half), shape(MESSAGE, BLK), shape(MESSAGE, BLK)),
        in_specs=[HBM, HBM] + [VMEM] * 4,
        out_specs=(VMEM,) * 3,
        scratch_shapes=[osmem, stiff_scratch(FACE_BLOCKS), DMA, DMA],
        compiler_params=params(12),
        cost_estimate=cost(3, 1),
        name="faces",
    )(order, stiff, lbuf, cbuf, wbd, zpart)
    za, zb = pl.pallas_call(
        join_kernel,
        out_shape=(shape(MESSAGE, BLK), shape(MESSAGE, BLK)),
        in_specs=[VMEM] * 4,
        out_specs=(VMEM,) * 2,
        input_output_aliases={0: 0, 1: 1},
        compiler_params=params(2),
        cost_estimate=cost(0.1, 0.1),
        name="join",
    )(za, zb, fya, fyb)
    fzb = exchange(zb, "gz", 1)
    fza = exchange(za, "gz", 0)
    wef, yea, yeb, xa, xb, keep = pl.pallas_call(
        side_kernel,
        out_shape=(
            shape(rows, 512, dtype=half),
            shape(4 * BLK, BLK),
            shape(4 * BLK, BLK),
            shape(BLK, BLK),
            shape(BLK, BLK),
            shape(len(KEPT) * BLK, BLK),
        ),
        in_specs=[HBM, HBM] + [VMEM] * 4,
        out_specs=(VMEM,) * 6,
        scratch_shapes=[osmem, stiff_scratch(SIDE_BLOCKS), DMA, DMA],
        compiler_params=params(12),
        cost_estimate=cost(3, 1),
        name="sides",
    )(order, stiff, lbuf, cbuf, wbd, za)
    fyea = exchange(yea, "gy", 0)
    fyeb = exchange(yeb, "gy", 1)
    fxa = exchange(xa, "gx", 0)
    fxb = exchange(xb, "gx", 1)
    out = pl.pallas_call(
        rest_kernel,
        out_shape=shape(size, size),
        in_specs=[HBM, HBM] + [VMEM] * 4,
        out_specs=HBM,
        scratch_shapes=[
            osmem,
            stiff_scratch(REST_BLOCKS),
            pltpu.VMEM((PAN, rows), half),
            pltpu.VMEM((2 * (len(KEPT) + len(REST_BLOCKS)) * BLK, BLK), jnp.float32),
            DMA,
            DMA,
            DMA,
        ],
        compiler_params=params(16),
        cost_estimate=cost(3, 8),
        name="rest",
    )(order, stiff, wbd, wac, wef, keep)
    out = pl.pallas_call(
        last_kernel,
        out_shape=shape(size, size),
        in_specs=[HBM] + [VMEM] * 12 + [HBM],
        out_specs=HBM,
        scratch_shapes=[osmem, pltpu.VMEM((48 * BLK, BLK), jnp.float32), DMA, DMA],
        input_output_aliases={13: 0},
        compiler_params=params(12),
        cost_estimate=cost(0.1, 3),
        name="last",
    )(order, za, zb, fza, fzb, yea, yeb, fyea, fyeb, xa, xb, fxa, fxb, out)
    return out.reshape(1, 1, 1, size, size)


def solution(mesh):
    return jax.shard_map(
        shards,
        mesh=mesh,
        in_specs=(
            P("gx", "gy", "gz", None, None),
            P("gx", "gy", "gz", None, None),
            P("gx", "gy", "gz", None, None),
            P("gx", "gy", "gz", None),
        ),
        out_specs=P("gx", "gy", "gz", None, None),
        check_vma=False,
    )
```

```python
import jax
import jax.numpy as jnp
from jax import lax
from jax.experimental import pallas as pl
from jax.experimental.pallas import tpu as pltpu
from jax.sharding import PartitionSpec as P

BLK = 128
NBLK = 12
PAN = 256

PAIRS = {"A": (4, 5), "B": (8, 9), "C": (6, 7), "D": (10, 11), "E": (2, 3), "F": (0, 1)}
COLUMNS = (8, 9, 10, 11, 4, 5, 6, 7, 2, 3, 0, 1)
Z_HIGH, Z_LOW = ((6, 7), (6, 10), (6, 11), (7, 10), (7, 11), (10, 11)), ((4, 5), (4, 8), (4, 9), (5, 8), (5, 9), (8, 9))
Z_HIGH_PACK, Z_LOW_PACK = ((6, 7), (11, 10)), ((4, 5), (8, 9))
Y_HIGH, Y_LOW = ((3, 3), (3, 9), (3, 11), (9, 11)), ((2, 2), (2, 8), (2, 10), (8, 10))
KEPT = ((2, 3), (2, 9), (3, 8), (2, 11), (3, 10), (8, 11), (9, 10), (0, 1))
FACES = 8 * BLK
MESSAGE = FACES + 8


def position(order, k):
    if k < 2:
        at = k ^ (lax.axis_index("gx") % 2)
    elif k < 4:
        at = 2 + ((k - 2) ^ (lax.axis_index("gy") % 2))
    elif k < 8:
        at = 4 + ((k - 4) ^ (2 * (lax.axis_index("gz") % 2)))
    else:
        at = 8 + ((k - 8) ^ (lax.axis_index("gy") % 2 + 2 * (lax.axis_index("gz") % 2)))
    return pl.multiple_of(order[at] * BLK, BLK)


def positions(order):
    return [position(order, k) for k in range(NBLK)]


def fetch_order(order, osmem, sem):
    copy = pltpu.make_async_copy(order, osmem, sem)
    copy.start()
    return copy


def stiff_copies(at, stiff, buf, sem, blocks):
    return [
        pltpu.make_async_copy(
            stiff.at[pl.ds(at[k], BLK), pl.ds(at[l], BLK)], buf.at[pl.ds(n * BLK, BLK), :], sem
        )
        for n, (k, l) in enumerate(blocks)
    ]


def weigh(lbuf, cbuf, columns, pan):
    depth = (pan + 1) * PAN
    return jnp.dot(
        lbuf[pan * PAN : depth, :depth], cbuf[:depth, columns], preferred_element_type=jnp.float32
    ).astype(jnp.bfloat16)


def gram(left, right):
    return lax.dot_general(left, right, (((0,), (0,)), ((), ())), preferred_element_type=jnp.float32)


def rows_ge():
    r = lax.broadcasted_iota(jnp.int32, (BLK, BLK), 0)
    c = lax.broadcasted_iota(jnp.int32, (BLK, BLK), 1)
    return r, c


def pack(first, second):
    r, c = rows_ge()
    return jnp.where(r <= c, first, second), jnp.sum(jnp.where(r == c, second, 0.0), axis=0, keepdims=True)


def unpack(tile, diagonal):
    r, c = rows_ge()
    turned = tile.T
    first = jnp.where(r <= c, tile, turned)
    return first, jnp.where(r > c, tile, jnp.where(r < c, turned, diagonal))


def two_rows(first, second):
    row = lax.broadcasted_iota(jnp.int32, (8, BLK), 0)
    return jnp.where(row == 0, first, jnp.where(row == 1, second, 0.0))


def piece(result, i, j):
    return result[i * BLK : (i + 1) * BLK, j * BLK : (j + 1) * BLK]


def slot(n):
    return slice(n * BLK, (n + 1) * BLK)


FACE_BLOCKS = ((4, 4), (4, 5), (5, 5), (4, 8), (4, 9), (5, 8), (5, 9), (6, 6), (6, 7), (7, 7), (6, 10), (6, 11), (7, 10), (7, 11))
SIDE_BLOCKS = tuple((k, l) for k in (2, 3) for l in (2, 3, 8, 9, 10, 11) if k <= l) + ((8, 10), (8, 11), (9, 10), (9, 11), (0, 0), (0, 1), (1, 1))
REST = (
    ("F", (("bd", (8, 9, 10, 11)), ("ac", (4, 5, 6, 7)), ("e", (2, 3)))),
    ("E", (("ac", (4, 5, 6, 7)),)),
    ("A", (("c", (6, 7)), ("d", (10, 11)))),
    ("C", (("b", (8, 9)),)),
)
REST_BLOCKS = tuple((k, l) for left, rights in REST for _, cols in rights for k in PAIRS[left] for l in cols)
LATER = FACE_BLOCKS + SIDE_BLOCKS + REST_BLOCKS
AT_FACES, AT_SIDES, AT_REST = 0, len(FACE_BLOCKS), len(FACE_BLOCKS) + len(SIDE_BLOCKS)
EDGE_BLOCKS = ((8, 8), (8, 9), (9, 9), (10, 10), (10, 11), (11, 11))


def edge_kernel(order, inverse, coupling, stiff, lbuf, cbuf, sall, wbd, yda, ydb, zpart, osmem, sbuf, osem, lsem, csem, rsem, ssem):
    fetch = fetch_order(order, osmem, osem)
    panels = lbuf.shape[0] // PAN
    lcopies = [
        pltpu.make_async_copy(
            inverse.at[pl.ds(pan * PAN, PAN), pl.ds(0, (pan + 1) * PAN)],
            lbuf.at[pl.ds(pan * PAN, PAN), pl.ds(0, (pan + 1) * PAN)],
            lsem.at[pan],
        )
        for pan in range(panels)
    ]
    for copy in lcopies[:2]:
        copy.start()
    fetch.wait()
    at = positions(osmem)
    ccopies = []
    for pan in range(panels):
        rows = pl.ds(pan * PAN, PAN)
        group = [
            pltpu.make_async_copy(
                coupling.at[rows, pl.ds(at[k], BLK)], cbuf.at[rows, pl.ds(n * BLK, BLK)], csem.at[pan]
            )
            for n, k in enumerate(COLUMNS[:4])
        ]
        ccopies.append(group)
        if pan >= 2:
            lcopies[pan].start()
        for copy in group:
            copy.start()
    scopies = stiff_copies(at, stiff, sbuf, ssem, EDGE_BLOCKS)
    for copy in scopies:
        copy.start()
    later = [
        pltpu.make_async_copy(
            coupling.at[:, pl.ds(at[k], BLK)], cbuf.at[:, pl.ds((n + 4) * BLK, BLK)], rsem
        )
        for n, k in enumerate(COLUMNS[4:])
    ]
    later += stiff_copies(at, stiff, sall, rsem, LATER)
    for pan in range(panels):
        lcopies[pan].wait()
        for copy in ccopies[pan]:
            copy.wait()
        if pan == 2:
            for copy in later:
                copy.start()
        wbd[pan * PAN : (pan + 1) * PAN, :] = weigh(lbuf, cbuf, slice(0, 512), pan)
    for copy in scopies:
        copy.wait()
    full = []
    for n in range(2):
        half = wbd[:, n * 256 : (n + 1) * 256]
        result = gram(half, half)
        for m, (i, j) in enumerate(((0, 0), (0, 1), (1, 1))):
            full.append(sbuf[slot(n * 3 + m)].astype(jnp.float32) - piece(result, i, j))
    b8, b89, b9, b10, b1011, b11 = full
    ydb[:BLK], row = pack(b8, b10)
    ydb[BLK:] = two_rows(row, 0.0)
    yda[:BLK], row = pack(b11, b9)
    yda[BLK:] = two_rows(row, 0.0)
    zpart[slot(0)] = b89
    zpart[slot(1)] = b1011
    zpart[slot(2)], low = pack(b8, b9)
    zpart[slot(3)], high = pack(b11, b10)
    zpart[4 * BLK :] = two_rows(low, high)
    for copy in later:
        copy.wait()


def face_kernel(sall, lbuf, cbuf, wbd, zpart, wac, za, zb):
    for pan in range(lbuf.shape[0] // PAN):
        wac[pan * PAN : (pan + 1) * PAN, :] = weigh(lbuf, cbuf, slice(512, 1024), pan)
    for n, (out, part) in enumerate(((zb, 0), (za, 1))):
        own = wac[:, n * 256 : (n + 1) * 256]
        inner = gram(own, own)
        outer = gram(own, wbd[:, n * 256 : (n + 1) * 256])
        base = AT_FACES + n * 7

        def value(m, result, i, j):
            return sall[slot(base + m)].astype(jnp.float32) - piece(result, i, j)

        out[slot(6)], row = pack(value(0, inner, 0, 0), value(2, inner, 1, 1))
        out[slot(0)] = value(1, inner, 0, 1)
        for m, (i, j) in enumerate(((0, 0), (0, 1), (1, 0), (1, 1))):
            out[slot(1 + m)] = value(3 + m, outer, i, j)
        out[slot(5)] = zpart[slot(part)]
        out[slot(7)] = zpart[slot(2 + part)]
        out[FACES:] = two_rows(row, zpart[4 * BLK + part : 4 * BLK + part + 1])


def join_kernel(za, zb, fya, fyb, za_out, zb_out):
    del za, zb
    r, c = rows_ge()
    above = r <= c
    row = lax.broadcasted_iota(jnp.int32, (8, BLK), 0) == 1
    za_out[slot(7)] = za_out[slot(7)] + jnp.where(above, fya[:BLK], fyb[:BLK])
    za_out[FACES:] = za_out[FACES:] + jnp.where(row, fyb[BLK : BLK + 1], 0.0)
    zb_out[slot(7)] = zb_out[slot(7)] + jnp.where(above, fyb[:BLK], fya[:BLK])
    zb_out[FACES:] = zb_out[FACES:] + jnp.where(row, fya[BLK : BLK + 1], 0.0)


def side_kernel(sall, lbuf, cbuf, wbd, after, wef, yea, yeb, xa, xb, keep):
    del after
    for pan in range(lbuf.shape[0] // PAN):
        wef[pan * PAN : (pan + 1) * PAN, :] = weigh(lbuf, cbuf, slice(1024, 1536), pan)
    e, f = wef[:, :256], wef[:, 256:]
    targets = {pair: (yea, n) for n, pair in enumerate(Y_HIGH)} | {pair: (yeb, n) for n, pair in enumerate(Y_LOW)}
    targets |= {pair: (keep, n) for n, pair in enumerate(KEPT)} | {(1, 1): (xa, 0), (0, 0): (xb, 0)}

    def emit(result, rows, cols):
        for i, k in enumerate(rows):
            for j, l in enumerate(cols):
                if k <= l:
                    out, n = targets[(k, l)]
                    m = AT_SIDES + SIDE_BLOCKS.index((k, l))
                    out[slot(n)] = sall[slot(m)].astype(jnp.float32) - piece(result, i, j)

    emit(gram(e, e), (2, 3), (2, 3))
    emit(gram(e, wbd[...]), (2, 3), (8, 9, 10, 11))
    emit(gram(wbd[:, :256], wbd[:, 256:]), (8, 9), (10, 11))
    emit(gram(f, f), (0, 1), (0, 1))


class Writer:
    def __init__(self, order, osmem, osem, out, stage, sem):
        self.fetch = fetch_order(order, osmem, osem)
        self.osmem, self.out, self.stage, self.sem = osmem, out, stage, sem
        self.cells, self.copies, self.at = [], [], None

    def ready(self):
        self.fetch.wait()
        self.at = positions(self.osmem)
        self.flush()

    def flush(self):
        if self.at is not None:
            for n in range(len(self.copies), len(self.cells)):
                k, l = self.cells[n]
                copy = pltpu.make_async_copy(
                    self.stage.at[pl.ds(n * BLK, BLK), :],
                    self.out.at[pl.ds(self.at[k], BLK), pl.ds(self.at[l], BLK)],
                    self.sem,
                )
                copy.start()
                self.copies.append(copy)

    def emit(self, k, l, value):
        self.stage[slot(len(self.cells))] = value
        self.cells.append((k, l))
        if k != l:
            self.stage[slot(len(self.cells))] = value.T
            self.cells.append((l, k))
        self.flush()

    def finish(self):
        for copy in self.copies:
            copy.wait()


def rest_kernel(order, sall, wbd, wac, wef, keep, out, osmem, turned, stage, osem, wsem):
    writer = Writer(order, osmem, osem, out, stage, wsem)
    whole = {"ac": (wac, 0, 512), "bd": (wbd, 0, 512), "e": (wef, 0, 256), "f": (wef, 256, 512), "a": (wac, 0, 256)}
    whole |= {"c": (wac, 256, 512), "b": (wbd, 0, 256), "d": (wbd, 256, 512)}
    for n, (k, l) in enumerate(KEPT):
        writer.emit(k, l, keep[slot(n)])
    m = AT_REST
    for left, rights in REST:
        ref, lo, hi = whole[left.lower()]
        turned[...] = ref[:, lo:hi].T
        for name, cols in rights:
            ref, lo, hi = whole[name]
            result = jnp.dot(turned[...], ref[:, lo:hi], preferred_element_type=jnp.float32)
            if writer.at is None:
                writer.ready()
            for i, k in enumerate(PAIRS[left]):
                for j, l in enumerate(cols):
                    writer.emit(k, l, sall[slot(m)].astype(jnp.float32) - piece(result, i, j))
                    m += 1
    writer.finish()


def last_kernel(order, za, zb, fza, fzb, yea, yeb, fyea, fyeb, xa, xb, fxa, fxb, before, out, osmem, stage, osem, wsem):
    del before
    writer = Writer(order, osmem, osem, out, stage, wsem)
    for pairs, packs, own, other in ((Z_LOW, Z_LOW_PACK, zb, fzb), (Z_HIGH, Z_HIGH_PACK, za, fza)):
        for n, (k, l) in enumerate(pairs):
            writer.emit(k, l, own[slot(n)] + other[slot(n)])
        for n, (k, l) in enumerate(packs):
            row = slice(FACES + n, FACES + n + 1)
            first, second = unpack(own[slot(6 + n)] + other[slot(6 + n)], own[row] + other[row])
            writer.emit(k, k, first)
            writer.emit(l, l, second)
        if writer.at is None:
            writer.ready()
    for pairs, own, other in ((Y_HIGH, yea, fyea), (Y_LOW, yeb, fyeb)):
        for n, (k, l) in enumerate(pairs):
            writer.emit(k, l, own[slot(n)] + other[slot(n)])
    writer.emit(0, 0, xb[...] + fxb[...])
    writer.emit(1, 1, xa[...] + fxa[...])
    writer.finish()


def exchange(value, axis, start):
    size = lax.axis_size(axis)
    pairs = [(i, i + 1) for i in range(start, size - 1, 2)]
    return lax.ppermute(value, axis, pairs + [(j, i) for i, j in pairs])


HBM = pl.BlockSpec(memory_space=pltpu.HBM)
VMEM = pl.BlockSpec(memory_space=pltpu.VMEM)
DMA = pltpu.SemaphoreType.DMA


def shape(*dims, dtype=jnp.float32):
    return jax.ShapeDtypeStruct(dims, dtype)


def params(mib):
    return pltpu.CompilerParams(vmem_limit_bytes=mib * 1024 * 1024)


def cost(gigaflops, megabytes):
    return pl.CostEstimate(
        flops=int(gigaflops * 1e9), bytes_accessed=int(megabytes * 1e6), transcendentals=0
    )


def in_hbm(value):
    return pltpu.with_memory_space_constraint(value, pltpu.HBM)


def shards(inv_factor, coupling, stiff_gg, block_order):
    rows = inv_factor.shape[3]
    size = NBLK * BLK
    half = jnp.bfloat16
    order = in_hbm(block_order.reshape(NBLK))
    inverse = in_hbm(inv_factor.reshape(rows, rows))
    coupled = in_hbm(coupling.reshape(rows, size))
    stiff = in_hbm(stiff_gg.reshape(size, size))
    panels = rows // PAN
    osmem = pltpu.SMEM((NBLK,), jnp.int32)

    lbuf, cbuf, sall, wbd, yda, ydb, zpart = pl.pallas_call(
        edge_kernel,
        out_shape=(
            shape(rows, rows, dtype=half),
            shape(rows, size, dtype=half),
            shape(len(LATER) * BLK, BLK, dtype=half),
            shape(rows, 512, dtype=half),
            shape(BLK + 8, BLK),
            shape(BLK + 8, BLK),
            shape(4 * BLK + 8, BLK),
        ),
        in_specs=[HBM] * 4,
        out_specs=(VMEM,) * 7,
        scratch_shapes=[osmem, pltpu.VMEM((len(EDGE_BLOCKS) * BLK, BLK), half), DMA, DMA((panels,)), DMA((panels,)), DMA, DMA],
        compiler_params=params(12),
        cost_estimate=cost(3, 8),
        name="edges",
    )(order, inverse, coupled, stiff)
    fya = exchange(yda, "gy", 0)
    fyb = exchange(ydb, "gy", 1)
    wac, za, zb = pl.pallas_call(
        face_kernel,
        out_shape=(shape(rows, 512, dtype=half), shape(MESSAGE, BLK), shape(MESSAGE, BLK)),
        in_specs=[VMEM] * 5,
        out_specs=(VMEM,) * 3,
        compiler_params=params(12),
        cost_estimate=cost(3, 1),
        name="faces",
    )(sall, lbuf, cbuf, wbd, zpart)
    za, zb = pl.pallas_call(
        join_kernel,
        out_shape=(shape(MESSAGE, BLK), shape(MESSAGE, BLK)),
        in_specs=[VMEM] * 4,
        out_specs=(VMEM,) * 2,
        input_output_aliases={0: 0, 1: 1},
        compiler_params=params(2),
        cost_estimate=cost(0.1, 0.1),
        name="join",
    )(za, zb, fya, fyb)
    fzb = exchange(zb, "gz", 1)
    fza = exchange(za, "gz", 0)
    wef, yea, yeb, xa, xb, keep = pl.pallas_call(
        side_kernel,
        out_shape=(
            shape(rows, 512, dtype=half),
            shape(4 * BLK, BLK),
            shape(4 * BLK, BLK),
            shape(BLK, BLK),
            shape(BLK, BLK),
            shape(len(KEPT) * BLK, BLK),
        ),
        in_specs=[VMEM] * 5,
        out_specs=(VMEM,) * 6,
        compiler_params=params(12),
        cost_estimate=cost(3, 1),
        name="sides",
    )(sall, lbuf, cbuf, wbd, za)
    fyea = exchange(yea, "gy", 0)
    fyeb = exchange(yeb, "gy", 1)
    fxa = exchange(xa, "gx", 0)
    fxb = exchange(xb, "gx", 1)
    out = pl.pallas_call(
        rest_kernel,
        out_shape=shape(size, size),
        in_specs=[HBM] + [VMEM] * 5,
        out_specs=HBM,
        scratch_shapes=[
            osmem,
            pltpu.VMEM((PAN, rows), half),
            pltpu.VMEM((2 * (len(KEPT) + len(REST_BLOCKS)) * BLK, BLK), jnp.float32),
            DMA,
            DMA,
        ],
        compiler_params=params(16),
        cost_estimate=cost(3, 8),
        name="rest",
    )(order, sall, wbd, wac, wef, keep)
    out = pl.pallas_call(
        last_kernel,
        out_shape=shape(size, size),
        in_specs=[HBM] + [VMEM] * 12 + [HBM],
        out_specs=HBM,
        scratch_shapes=[osmem, pltpu.VMEM((48 * BLK, BLK), jnp.float32), DMA, DMA],
        input_output_aliases={13: 0},
        compiler_params=params(12),
        cost_estimate=cost(0.1, 3),
        name="last",
    )(order, za, zb, fza, fzb, yea, yeb, fyea, fyeb, xa, xb, fxa, fxb, out)
    return out.reshape(1, 1, 1, size, size)


def solution(mesh):
    return jax.shard_map(
        shards,
        mesh=mesh,
        in_specs=(
            P("gx", "gy", "gz", None, None),
            P("gx", "gy", "gz", None, None),
            P("gx", "gy", "gz", None, None),
            P("gx", "gy", "gz", None),
        ),
        out_specs=P("gx", "gy", "gz", None, None),
        check_vma=False,
    )
```

```python
import jax
import jax.numpy as jnp
from jax import lax
from jax.experimental import pallas as pl
from jax.experimental.pallas import tpu as pltpu
from jax.sharding import PartitionSpec as P

BLK = 128
NBLK = 12
PAN = 256

PAIRS = {"A": (4, 5), "B": (8, 9), "C": (6, 7), "D": (10, 11), "E": (2, 3), "F": (0, 1)}
COLUMNS = (8, 9, 10, 11, 4, 5, 6, 7, 2, 3, 0, 1)
Z_HIGH, Z_LOW = ((6, 7), (6, 10), (6, 11), (7, 10), (7, 11), (10, 11)), ((4, 5), (4, 8), (4, 9), (5, 8), (5, 9), (8, 9))
Z_HIGH_PACK, Z_LOW_PACK = ((6, 7), (11, 10)), ((4, 5), (8, 9))
Y_HIGH, Y_LOW = ((3, 3), (3, 9), (3, 11), (9, 11)), ((2, 2), (2, 8), (2, 10), (8, 10))
KEPT = ((2, 3), (2, 9), (3, 8), (2, 11), (3, 10), (8, 11), (9, 10), (0, 1))
FACES = 8 * BLK
MESSAGE = FACES + 8


def position(order, k):
    if k < 2:
        at = k ^ (lax.axis_index("gx") % 2)
    elif k < 4:
        at = 2 + ((k - 2) ^ (lax.axis_index("gy") % 2))
    elif k < 8:
        at = 4 + ((k - 4) ^ (2 * (lax.axis_index("gz") % 2)))
    else:
        at = 8 + ((k - 8) ^ (lax.axis_index("gy") % 2 + 2 * (lax.axis_index("gz") % 2)))
    return pl.multiple_of(order[at] * BLK, BLK)


def positions(order):
    return [position(order, k) for k in range(NBLK)]


def fetch_order(order, osmem, sem):
    copy = pltpu.make_async_copy(order, osmem, sem)
    copy.start()
    return copy


def stiff_copies(at, stiff, buf, sem, blocks):
    return [
        pltpu.make_async_copy(
            stiff.at[pl.ds(at[k], BLK), pl.ds(at[l], BLK)], buf.at[pl.ds(n * BLK, BLK), :], sem
        )
        for n, (k, l) in enumerate(blocks)
    ]


def weigh(lbuf, cbuf, columns, pan):
    depth = (pan + 1) * PAN
    return jnp.dot(
        lbuf[pan * PAN : depth, :depth], cbuf[:depth, columns], preferred_element_type=jnp.float32
    ).astype(jnp.bfloat16)


def gram(left, right):
    return lax.dot_general(left, right, (((0,), (0,)), ((), ())), preferred_element_type=jnp.float32)


def rows_ge():
    r = lax.broadcasted_iota(jnp.int32, (BLK, BLK), 0)
    c = lax.broadcasted_iota(jnp.int32, (BLK, BLK), 1)
    return r, c


def pack(first, second):
    r, c = rows_ge()
    return jnp.where(r <= c, first, second), jnp.sum(jnp.where(r == c, second, 0.0), axis=0, keepdims=True)


def unpack(tile, diagonal):
    r, c = rows_ge()
    turned = tile.T
    first = jnp.where(r <= c, tile, turned)
    return first, jnp.where(r > c, tile, jnp.where(r < c, turned, diagonal))


def two_rows(first, second):
    row = lax.broadcasted_iota(jnp.int32, (8, BLK), 0)
    return jnp.where(row == 0, first, jnp.where(row == 1, second, 0.0))


def piece(result, i, j):
    return result[i * BLK : (i + 1) * BLK, j * BLK : (j + 1) * BLK]


def slot(n):
    return slice(n * BLK, (n + 1) * BLK)


FACE_BLOCKS = ((4, 4), (4, 5), (5, 5), (4, 8), (4, 9), (5, 8), (5, 9), (6, 6), (6, 7), (7, 7), (6, 10), (6, 11), (7, 10), (7, 11))
SIDE_BLOCKS = tuple((k, l) for k in (2, 3) for l in (2, 3, 8, 9, 10, 11) if k <= l) + ((8, 10), (8, 11), (9, 10), (9, 11), (0, 0), (0, 1), (1, 1))
REST = (
    ("F", (("bd", (8, 9, 10, 11)), ("ac", (4, 5, 6, 7)), ("e", (2, 3)))),
    ("E", (("ac", (4, 5, 6, 7)),)),
    ("A", (("c", (6, 7)), ("d", (10, 11)))),
    ("C", (("b", (8, 9)),)),
)
REST_BLOCKS = tuple((k, l) for left, rights in REST for _, cols in rights for k in PAIRS[left] for l in cols)
LATER = FACE_BLOCKS + SIDE_BLOCKS + REST_BLOCKS
AT_FACES, AT_SIDES, AT_REST = 0, len(FACE_BLOCKS), len(FACE_BLOCKS) + len(SIDE_BLOCKS)
EDGE_BLOCKS = ((8, 8), (8, 9), (9, 9), (10, 10), (10, 11), (11, 11))


def edge_kernel(order, inverse, coupling, stiff, lbuf, cbuf, sall, wbd, yda, ydb, zpart, osmem, sbuf, osem, lsem, csem, rsem, ssem):
    fetch = fetch_order(order, osmem, osem)
    panels = lbuf.shape[0] // PAN
    lcopies = [
        pltpu.make_async_copy(
            inverse.at[pl.ds(pan * PAN, PAN), pl.ds(0, (pan + 1) * PAN)],
            lbuf.at[pl.ds(pan * PAN, PAN), pl.ds(0, (pan + 1) * PAN)],
            lsem.at[pan],
        )
        for pan in range(panels)
    ]
    for copy in lcopies:
        copy.start()
    fetch.wait()
    at = positions(osmem)
    ccopies = []
    for pan in range(panels):
        rows = pl.ds(pan * PAN, PAN)
        group = [
            pltpu.make_async_copy(
                coupling.at[rows, pl.ds(at[k], BLK)], cbuf.at[rows, pl.ds(n * BLK, BLK)], csem.at[pan]
            )
            for n, k in enumerate(COLUMNS[:4])
        ]
        ccopies.append(group)
        for copy in group:
            copy.start()
    scopies = stiff_copies(at, stiff, sbuf, ssem, EDGE_BLOCKS)
    for copy in scopies:
        copy.start()
    later = [
        pltpu.make_async_copy(
            coupling.at[:, pl.ds(at[k], BLK)], cbuf.at[:, pl.ds((n + 4) * BLK, BLK)], rsem
        )
        for n, k in enumerate(COLUMNS[4:])
    ]
    later += stiff_copies(at, stiff, sall, rsem, LATER)
    for pan in range(panels):
        lcopies[pan].wait()
        for copy in ccopies[pan]:
            copy.wait()
        if pan == 0:
            for copy in later:
                copy.start()
        wbd[pan * PAN : (pan + 1) * PAN, :] = weigh(lbuf, cbuf, slice(0, 512), pan)
    for copy in scopies:
        copy.wait()
    full = []
    for n in range(2):
        half = wbd[:, n * 256 : (n + 1) * 256]
        result = gram(half, half)
        for m, (i, j) in enumerate(((0, 0), (0, 1), (1, 1))):
            full.append(sbuf[slot(n * 3 + m)].astype(jnp.float32) - piece(result, i, j))
    b8, b89, b9, b10, b1011, b11 = full
    ydb[:BLK], row = pack(b8, b10)
    ydb[BLK:] = two_rows(row, 0.0)
    yda[:BLK], row = pack(b11, b9)
    yda[BLK:] = two_rows(row, 0.0)
    zpart[slot(0)] = b89
    zpart[slot(1)] = b1011
    zpart[slot(2)], low = pack(b8, b9)
    zpart[slot(3)], high = pack(b11, b10)
    zpart[4 * BLK :] = two_rows(low, high)
    for copy in later:
        copy.wait()


def face_kernel(sall, lbuf, cbuf, wbd, zpart, wac, za, zb):
    for pan in range(lbuf.shape[0] // PAN):
        wac[pan * PAN : (pan + 1) * PAN, :] = weigh(lbuf, cbuf, slice(512, 1024), pan)
    for n, (out, part) in enumerate(((zb, 0), (za, 1))):
        own = wac[:, n * 256 : (n + 1) * 256]
        inner = gram(own, own)
        outer = gram(own, wbd[:, n * 256 : (n + 1) * 256])
        base = AT_FACES + n * 7

        def value(m, result, i, j):
            return sall[slot(base + m)].astype(jnp.float32) - piece(result, i, j)

        out[slot(6)], row = pack(value(0, inner, 0, 0), value(2, inner, 1, 1))
        out[slot(0)] = value(1, inner, 0, 1)
        for m, (i, j) in enumerate(((0, 0), (0, 1), (1, 0), (1, 1))):
            out[slot(1 + m)] = value(3 + m, outer, i, j)
        out[slot(5)] = zpart[slot(part)]
        out[slot(7)] = zpart[slot(2 + part)]
        out[FACES:] = two_rows(row, zpart[4 * BLK + part : 4 * BLK + part + 1])


def join_kernel(za, zb, fya, fyb, za_out, zb_out):
    del za, zb
    r, c = rows_ge()
    above = r <= c
    row = lax.broadcasted_iota(jnp.int32, (8, BLK), 0) == 1
    below, diagonal = known("gy", fyb[:BLK]), known("gy", fyb[BLK : BLK + 1])
    za_out[slot(7)] = za_out[slot(7)] + jnp.where(above, fya[:BLK], below)
    za_out[FACES:] = za_out[FACES:] + jnp.where(row, diagonal, 0.0)
    zb_out[slot(7)] = zb_out[slot(7)] + jnp.where(above, below, fya[:BLK])
    zb_out[FACES:] = zb_out[FACES:] + jnp.where(row, fya[BLK : BLK + 1], 0.0)


def side_kernel(sall, lbuf, cbuf, wbd, after, wef, yea, yeb, xa, xb, keep):
    del after
    for pan in range(lbuf.shape[0] // PAN):
        wef[pan * PAN : (pan + 1) * PAN, :] = weigh(lbuf, cbuf, slice(1024, 1536), pan)
    e, f = wef[:, :256], wef[:, 256:]
    targets = {pair: (yea, n) for n, pair in enumerate(Y_HIGH)} | {pair: (yeb, n) for n, pair in enumerate(Y_LOW)}
    targets |= {pair: (keep, n) for n, pair in enumerate(KEPT)} | {(1, 1): (xa, 0), (0, 0): (xb, 0)}

    def emit(result, rows, cols):
        for i, k in enumerate(rows):
            for j, l in enumerate(cols):
                if k <= l:
                    out, n = targets[(k, l)]
                    m = AT_SIDES + SIDE_BLOCKS.index((k, l))
                    out[slot(n)] = sall[slot(m)].astype(jnp.float32) - piece(result, i, j)

    emit(gram(e, e), (2, 3), (2, 3))
    emit(gram(e, wbd[...]), (2, 3), (8, 9, 10, 11))
    emit(gram(wbd[:, :256], wbd[:, 256:]), (8, 9), (10, 11))
    emit(gram(f, f), (0, 1), (0, 1))


class Writer:
    def __init__(self, order, osmem, osem, out, stage, sem):
        self.fetch = fetch_order(order, osmem, osem)
        self.osmem, self.out, self.stage, self.sem = osmem, out, stage, sem
        self.cells, self.copies, self.at = [], [], None

    def ready(self):
        self.fetch.wait()
        self.at = positions(self.osmem)
        self.flush()

    def flush(self):
        if self.at is not None:
            for n in range(len(self.copies), len(self.cells)):
                k, l = self.cells[n]
                copy = pltpu.make_async_copy(
                    self.stage.at[pl.ds(n * BLK, BLK), :],
                    self.out.at[pl.ds(self.at[k], BLK), pl.ds(self.at[l], BLK)],
                    self.sem,
                )
                copy.start()
                self.copies.append(copy)

    def emit(self, k, l, value):
        self.stage[slot(len(self.cells))] = value
        self.cells.append((k, l))
        if k != l:
            self.stage[slot(len(self.cells))] = value.T
            self.cells.append((l, k))
        self.flush()

    def finish(self):
        for copy in self.copies:
            copy.wait()


def rest_kernel(order, sall, wbd, wac, wef, keep, out, osmem, turned, stage, osem, wsem):
    writer = Writer(order, osmem, osem, out, stage, wsem)
    whole = {"ac": (wac, 0, 512), "bd": (wbd, 0, 512), "e": (wef, 0, 256), "f": (wef, 256, 512), "a": (wac, 0, 256)}
    whole |= {"c": (wac, 256, 512), "b": (wbd, 0, 256), "d": (wbd, 256, 512)}
    for n, (k, l) in enumerate(KEPT):
        writer.emit(k, l, keep[slot(n)])
    m = AT_REST
    for left, rights in REST:
        ref, lo, hi = whole[left.lower()]
        turned[...] = ref[:, lo:hi].T
        for name, cols in rights:
            ref, lo, hi = whole[name]
            result = jnp.dot(turned[...], ref[:, lo:hi], preferred_element_type=jnp.float32)
            if writer.at is None:
                writer.ready()
            for i, k in enumerate(PAIRS[left]):
                for j, l in enumerate(cols):
                    writer.emit(k, l, sall[slot(m)].astype(jnp.float32) - piece(result, i, j))
                    m += 1
    writer.finish()


def last_kernel(order, za, zb, fza, fzb, yea, yeb, fyea, fyeb, xa, xb, fxa, fxb, before, out, osmem, stage, osem, wsem):
    del before
    writer = Writer(order, osmem, osem, out, stage, wsem)
    for pairs, packs, own, other, take in (
        (Z_LOW, Z_LOW_PACK, zb, fzb, lambda value: known("gz", value)),
        (Z_HIGH, Z_HIGH_PACK, za, fza, lambda value: value),
    ):
        for n, (k, l) in enumerate(pairs):
            writer.emit(k, l, own[slot(n)] + take(other[slot(n)]))
        for n, (k, l) in enumerate(packs):
            row = slice(FACES + n, FACES + n + 1)
            first, second = unpack(own[slot(6 + n)] + take(other[slot(6 + n)]), own[row] + take(other[row]))
            writer.emit(k, k, first)
            writer.emit(l, l, second)
        if writer.at is None:
            writer.ready()
    for n, (k, l) in enumerate(Y_HIGH):
        writer.emit(k, l, yea[slot(n)] + fyea[slot(n)])
    for n, (k, l) in enumerate(Y_LOW):
        writer.emit(k, l, yeb[slot(n)] + known("gy", fyeb[slot(n)]))
    writer.emit(0, 0, xb[...] + known("gx", fxb[...]))
    writer.emit(1, 1, xa[...] + fxa[...])
    writer.finish()


def exchange_high(value, axis):
    return lax.ppermute(value, axis, [(i, i ^ 1) for i in range(lax.axis_size(axis))])


def exchange_low(value, axis):
    size, across = lax.axis_size(axis), lax.axis_size("gx")
    if axis == "gx":
        return lax.ppermute(value, axis, [(i, size - 1 - i) for i in range(size)])
    pairs = []
    for x in range(across):
        for i in range(size):
            to = (x ^ 1, i) if i in (0, size - 1) else (x, ((i - 1) ^ 1) + 1)
            pairs.append((x * size + i, to[0] * size + to[1]))
    return lax.ppermute(value, ("gx", axis), pairs)


def known(axis, value):
    at = lax.axis_index(axis)
    return jnp.where((at > 0) & (at < lax.axis_size(axis) - 1), value, 0.0)


HBM = pl.BlockSpec(memory_space=pltpu.HBM)
VMEM = pl.BlockSpec(memory_space=pltpu.VMEM)
DMA = pltpu.SemaphoreType.DMA


def shape(*dims, dtype=jnp.float32):
    return jax.ShapeDtypeStruct(dims, dtype)


def params(mib):
    return pltpu.CompilerParams(vmem_limit_bytes=mib * 1024 * 1024)


def cost(gigaflops, megabytes):
    return pl.CostEstimate(
        flops=int(gigaflops * 1e9), bytes_accessed=int(megabytes * 1e6), transcendentals=0
    )


def in_hbm(value):
    return pltpu.with_memory_space_constraint(value, pltpu.HBM)


def shards(inv_factor, coupling, stiff_gg, block_order):
    rows = inv_factor.shape[3]
    size = NBLK * BLK
    half = jnp.bfloat16
    order = in_hbm(block_order.reshape(NBLK))
    inverse = in_hbm(inv_factor.reshape(rows, rows))
    coupled = in_hbm(coupling.reshape(rows, size))
    stiff = in_hbm(stiff_gg.reshape(size, size))
    panels = rows // PAN
    osmem = pltpu.SMEM((NBLK,), jnp.int32)

    lbuf, cbuf, sall, wbd, yda, ydb, zpart = pl.pallas_call(
        edge_kernel,
        out_shape=(
            shape(rows, rows, dtype=half),
            shape(rows, size, dtype=half),
            shape(len(LATER) * BLK, BLK, dtype=half),
            shape(rows, 512, dtype=half),
            shape(BLK + 8, BLK),
            shape(BLK + 8, BLK),
            shape(4 * BLK + 8, BLK),
        ),
        in_specs=[HBM] * 4,
        out_specs=(VMEM,) * 7,
        scratch_shapes=[osmem, pltpu.VMEM((len(EDGE_BLOCKS) * BLK, BLK), half), DMA, DMA((panels,)), DMA((panels,)), DMA, DMA],
        compiler_params=params(12),
        cost_estimate=cost(3, 8),
        name="edges",
    )(order, inverse, coupled, stiff)
    fya = exchange_high(yda, "gy")
    fyb = exchange_low(ydb, "gy")
    wac, za, zb = pl.pallas_call(
        face_kernel,
        out_shape=(shape(rows, 512, dtype=half), shape(MESSAGE, BLK), shape(MESSAGE, BLK)),
        in_specs=[VMEM] * 5,
        out_specs=(VMEM,) * 3,
        compiler_params=params(12),
        cost_estimate=cost(3, 1),
        name="faces",
    )(sall, lbuf, cbuf, wbd, zpart)
    za, zb = pl.pallas_call(
        join_kernel,
        out_shape=(shape(MESSAGE, BLK), shape(MESSAGE, BLK)),
        in_specs=[VMEM] * 4,
        out_specs=(VMEM,) * 2,
        input_output_aliases={0: 0, 1: 1},
        compiler_params=params(2),
        cost_estimate=cost(0.1, 0.1),
        name="join",
    )(za, zb, fya, fyb)
    fzb = exchange_low(zb, "gz")
    fza = exchange_high(za, "gz")
    wef, yea, yeb, xa, xb, keep = pl.pallas_call(
        side_kernel,
        out_shape=(
            shape(rows, 512, dtype=half),
            shape(4 * BLK, BLK),
            shape(4 * BLK, BLK),
            shape(BLK, BLK),
            shape(BLK, BLK),
            shape(len(KEPT) * BLK, BLK),
        ),
        in_specs=[VMEM] * 5,
        out_specs=(VMEM,) * 6,
        compiler_params=params(12),
        cost_estimate=cost(3, 1),
        name="sides",
    )(sall, lbuf, cbuf, wbd, za)
    fyea = exchange_high(yea, "gy")
    fyeb = exchange_low(yeb, "gy")
    fxa = exchange_high(xa, "gx")
    fxb = exchange_low(xb, "gx")
    out = pl.pallas_call(
        rest_kernel,
        out_shape=shape(size, size),
        in_specs=[HBM] + [VMEM] * 5,
        out_specs=HBM,
        scratch_shapes=[
            osmem,
            pltpu.VMEM((PAN, rows), half),
            pltpu.VMEM((2 * (len(KEPT) + len(REST_BLOCKS)) * BLK, BLK), jnp.float32),
            DMA,
            DMA,
        ],
        compiler_params=params(16),
        cost_estimate=cost(3, 8),
        name="rest",
    )(order, sall, wbd, wac, wef, keep)
    out = pl.pallas_call(
        last_kernel,
        out_shape=shape(size, size),
        in_specs=[HBM] + [VMEM] * 12 + [HBM],
        out_specs=HBM,
        scratch_shapes=[osmem, pltpu.VMEM((48 * BLK, BLK), jnp.float32), DMA, DMA],
        input_output_aliases={13: 0},
        compiler_params=params(12),
        cost_estimate=cost(0.1, 3),
        name="last",
    )(order, za, zb, fza, fzb, yea, yeb, fyea, fyeb, xa, xb, fxa, fxb, out)
    return out.reshape(1, 1, 1, size, size)


def solution(mesh):
    return jax.shard_map(
        shards,
        mesh=mesh,
        in_specs=(
            P("gx", "gy", "gz", None, None),
            P("gx", "gy", "gz", None, None),
            P("gx", "gy", "gz", None, None),
            P("gx", "gy", "gz", None),
        ),
        out_specs=P("gx", "gy", "gz", None, None),
        check_vma=False,
    )
```

```python
import jax
import jax.numpy as jnp
from jax import lax
from jax.experimental import pallas as pl
from jax.experimental.pallas import tpu as pltpu
from jax.sharding import PartitionSpec as P


BLK = 128
NBLK = 12
PAN = 256

PAIRS = {"A": (4, 5), "B": (8, 9), "C": (6, 7), "D": (10, 11), "E": (2, 3), "F": (0, 1)}
COLUMNS = (8, 9, 10, 11, 4, 5, 6, 7, 2, 3, 0, 1)
Z_HIGH, Z_LOW = ((6, 7), (6, 10), (6, 11), (7, 10), (7, 11), (10, 11)), ((4, 5), (4, 8), (4, 9), (5, 8), (5, 9), (8, 9))
Z_HIGH_PACK, Z_LOW_PACK = ((6, 7), (11, 10)), ((4, 5), (8, 9))
Y_HIGH, Y_LOW = ((3, 3), (3, 9), (3, 11), (9, 11)), ((2, 2), (2, 8), (2, 10), (8, 10))
KEPT = ((2, 3), (2, 9), (3, 8), (2, 11), (3, 10), (8, 11), (9, 10), (0, 1))
FACES = 8 * BLK
GROUPS = ((0, 2), (2, 4), (4, 6))
MESSAGE = FACES + 8


def position(order, k):
    if k < 2:
        at = k ^ (lax.axis_index("gx") % 2)
    elif k < 4:
        at = 2 + ((k - 2) ^ (lax.axis_index("gy") % 2))
    elif k < 8:
        at = 4 + ((k - 4) ^ (2 * (lax.axis_index("gz") % 2)))
    else:
        at = 8 + ((k - 8) ^ (lax.axis_index("gy") % 2 + 2 * (lax.axis_index("gz") % 2)))
    return pl.multiple_of(order[at] * BLK, BLK)


def positions(order):
    return [position(order, k) for k in range(NBLK)]


def fetch_order(order, osmem, sem):
    copy = pltpu.make_async_copy(order, osmem, sem)
    copy.start()
    return copy


def stiff_copies(at, stiff, buf, sem, blocks):
    return [
        pltpu.make_async_copy(
            stiff.at[pl.ds(at[k], BLK), pl.ds(at[l], BLK)], buf.at[pl.ds(n * BLK, BLK), :], sem
        )
        for n, (k, l) in enumerate(blocks)
    ]


def weigh(lbuf, cbuf, columns, pan):
    depth = (pan + 1) * PAN
    return jnp.dot(
        lbuf[pan * PAN : depth, :depth], cbuf[:depth, columns], preferred_element_type=jnp.float32
    ).astype(jnp.bfloat16)


def gram(left, right):
    return lax.dot_general(left, right, (((0,), (0,)), ((), ())), preferred_element_type=jnp.float32)


def rows_ge():
    r = lax.broadcasted_iota(jnp.int32, (BLK, BLK), 0)
    c = lax.broadcasted_iota(jnp.int32, (BLK, BLK), 1)
    return r, c


def pack(first, second):
    r, c = rows_ge()
    return jnp.where(r <= c, first, second), jnp.sum(jnp.where(r == c, second, 0.0), axis=0, keepdims=True)


def unpack(tile, diagonal):
    r, c = rows_ge()
    turned = tile.T
    first = jnp.where(r <= c, tile, turned)
    return first, jnp.where(r > c, tile, jnp.where(r < c, turned, diagonal))


def two_rows(first, second):
    row = lax.broadcasted_iota(jnp.int32, (8, BLK), 0)
    return jnp.where(row == 0, first, jnp.where(row == 1, second, 0.0))


def piece(result, i, j):
    return result[i * BLK : (i + 1) * BLK, j * BLK : (j + 1) * BLK]


def slot(n):
    return slice(n * BLK, (n + 1) * BLK)


FACE_BLOCKS = ((4, 4), (4, 5), (5, 5), (4, 8), (4, 9), (5, 8), (5, 9), (6, 6), (6, 7), (7, 7), (6, 10), (6, 11), (7, 10), (7, 11))
SIDE_BLOCKS = tuple((k, l) for k in (2, 3) for l in (2, 3, 8, 9, 10, 11) if k <= l) + ((8, 10), (8, 11), (9, 10), (9, 11), (0, 0), (0, 1), (1, 1))
REST = (
    ("F", (("bd", (8, 9, 10, 11)), ("ac", (4, 5, 6, 7)), ("e", (2, 3)))),
    ("E", (("ac", (4, 5, 6, 7)),)),
    ("A", (("c", (6, 7)), ("d", (10, 11)))),
    ("C", (("b", (8, 9)),)),
)
REST_BLOCKS = tuple((k, l) for left, rights in REST for _, cols in rights for k in PAIRS[left] for l in cols)
LATER = FACE_BLOCKS + SIDE_BLOCKS + REST_BLOCKS
AT_FACES, AT_SIDES, AT_REST = 0, len(FACE_BLOCKS), len(FACE_BLOCKS) + len(SIDE_BLOCKS)
EDGE_BLOCKS = ((8, 8), (8, 9), (9, 9), (10, 10), (10, 11), (11, 11))


def edge_kernel(order, inverse, coupling, stiff, lbuf, cbuf, sall, wbd, yda, ydb, zpart, spots, osmem, sbuf, osem, lsem, csem, rsem, ssem):
    fetch = fetch_order(order, osmem, osem)
    panels = lbuf.shape[0] // PAN
    lcopies = [
        pltpu.make_async_copy(
            inverse.at[pl.ds(pan * PAN, PAN), pl.ds(0, (pan + 1) * PAN)],
            lbuf.at[pl.ds(pan * PAN, PAN), pl.ds(0, (pan + 1) * PAN)],
            lsem.at[pan],
        )
        for pan in range(panels)
    ]
    for copy in lcopies:
        copy.start()
    fetch.wait()
    at = positions(osmem)
    lane = lax.broadcasted_iota(jnp.int32, (8, BLK), 1)
    spots[...] = sum(jnp.where(lane == k, at[k], 0) for k in range(NBLK))
    ccopies = []
    for lo, hi in GROUPS:
        rows = pl.ds(lo * PAN, (hi - lo) * PAN)
        group = [
            pltpu.make_async_copy(
                coupling.at[rows, pl.ds(at[k], BLK)], cbuf.at[rows, pl.ds(n * BLK, BLK)], csem.at[lo]
            )
            for n, k in enumerate(COLUMNS[:4])
        ]
        ccopies.append(group)
        for copy in group:
            copy.start()
    scopies = stiff_copies(at, stiff, sbuf, ssem, EDGE_BLOCKS)
    for copy in scopies:
        copy.start()
    later = [
        pltpu.make_async_copy(
            coupling.at[:, pl.ds(at[k], BLK)], cbuf.at[:, pl.ds((n + 4) * BLK, BLK)], rsem
        )
        for n, k in enumerate(COLUMNS[4:])
    ]
    later += stiff_copies(at, stiff, sall, rsem, LATER)
    for (lo, hi), group in zip(GROUPS, ccopies):
        for pan in range(lo, hi):
            lcopies[pan].wait()
        for copy in group:
            copy.wait()
        if lo == 0:
            for copy in later:
                copy.start()
        for pan in range(lo, hi):
            wbd[pan * PAN : (pan + 1) * PAN, :] = weigh(lbuf, cbuf, slice(0, 512), pan)
    for copy in scopies:
        copy.wait()
    full = []
    for n in range(2):
        half = wbd[:, n * 256 : (n + 1) * 256]
        result = gram(half, half)
        for m, (i, j) in enumerate(((0, 0), (0, 1), (1, 1))):
            full.append(sbuf[slot(n * 3 + m)].astype(jnp.float32) - piece(result, i, j))
    b8, b89, b9, b10, b1011, b11 = full
    ydb[:BLK], row = pack(b8, b10)
    ydb[BLK:] = two_rows(row, 0.0)
    yda[:BLK], row = pack(b11, b9)
    yda[BLK:] = two_rows(row, 0.0)
    zpart[slot(0)] = b89
    zpart[slot(1)] = b1011
    zpart[slot(2)], low = pack(b8, b9)
    zpart[slot(3)], high = pack(b11, b10)
    zpart[4 * BLK :] = two_rows(low, high)
    for copy in later:
        copy.wait()


def face_kernel(sall, lbuf, cbuf, wbd, zpart, wac, za, zb):
    for pan in range(lbuf.shape[0] // PAN):
        wac[pan * PAN : (pan + 1) * PAN, :] = weigh(lbuf, cbuf, slice(512, 1024), pan)
    for n, (out, part) in enumerate(((zb, 0), (za, 1))):
        own = wac[:, n * 256 : (n + 1) * 256]
        inner = gram(own, own)
        outer = gram(own, wbd[:, n * 256 : (n + 1) * 256])
        base = AT_FACES + n * 7

        def value(m, result, i, j):
            return sall[slot(base + m)].astype(jnp.float32) - piece(result, i, j)

        out[slot(6)], row = pack(value(0, inner, 0, 0), value(2, inner, 1, 1))
        out[slot(0)] = value(1, inner, 0, 1)
        for m, (i, j) in enumerate(((0, 0), (0, 1), (1, 0), (1, 1))):
            out[slot(1 + m)] = value(3 + m, outer, i, j)
        out[slot(5)] = zpart[slot(part)]
        out[slot(7)] = zpart[slot(2 + part)]
        out[FACES:] = two_rows(row, zpart[4 * BLK + part : 4 * BLK + part + 1])


def join_kernel(za, zb, fya, fyb, za_out, zb_out):
    del za, zb
    r, c = rows_ge()
    above = r <= c
    row = lax.broadcasted_iota(jnp.int32, (8, BLK), 0) == 1
    below, diagonal = known("gy", fyb[:BLK]), known("gy", fyb[BLK : BLK + 1])
    za_out[slot(7)] = za_out[slot(7)] + jnp.where(above, fya[:BLK], below)
    za_out[FACES:] = za_out[FACES:] + jnp.where(row, diagonal, 0.0)
    zb_out[slot(7)] = zb_out[slot(7)] + jnp.where(above, below, fya[:BLK])
    zb_out[FACES:] = zb_out[FACES:] + jnp.where(row, fya[BLK : BLK + 1], 0.0)


def side_kernel(sall, lbuf, cbuf, wbd, after, wef, yea, yeb, xa, xb, keep):
    del after
    for pan in range(lbuf.shape[0] // PAN):
        wef[pan * PAN : (pan + 1) * PAN, :] = weigh(lbuf, cbuf, slice(1024, 1536), pan)
    e, f = wef[:, :256], wef[:, 256:]
    targets = {pair: (yea, n) for n, pair in enumerate(Y_HIGH)} | {pair: (yeb, n) for n, pair in enumerate(Y_LOW)}
    targets |= {pair: (keep, n) for n, pair in enumerate(KEPT)} | {(1, 1): (xa, 0), (0, 0): (xb, 0)}

    def emit(result, rows, cols):
        for i, k in enumerate(rows):
            for j, l in enumerate(cols):
                if k <= l:
                    out, n = targets[(k, l)]
                    m = AT_SIDES + SIDE_BLOCKS.index((k, l))
                    out[slot(n)] = sall[slot(m)].astype(jnp.float32) - piece(result, i, j)

    emit(gram(e, e), (2, 3), (2, 3))
    emit(gram(e, wbd[...]), (2, 3), (8, 9, 10, 11))
    emit(gram(wbd[:, :256], wbd[:, 256:]), (8, 9), (10, 11))
    emit(gram(f, f), (0, 1), (0, 1))


class Writer:
    def __init__(self, spots, out, stage, sem):
        row = spots[0:1, :]
        self.at = [pl.multiple_of(row[0, k], BLK) for k in range(NBLK)]
        self.out, self.stage, self.sem, self.copies = out, stage, sem, []

    def put(self, k, l, value):
        n = len(self.copies)
        self.stage[slot(n)] = value
        copy = pltpu.make_async_copy(
            self.stage.at[pl.ds(n * BLK, BLK), :],
            self.out.at[pl.ds(self.at[k], BLK), pl.ds(self.at[l], BLK)],
            self.sem,
        )
        copy.start()
        self.copies.append(copy)

    def emit(self, k, l, value):
        self.put(k, l, value)
        if k != l:
            self.put(l, k, value.T)

    def finish(self):
        for copy in self.copies:
            copy.wait()


def rest_kernel(spots, sall, wbd, wac, wef, keep, out, turned, stage, wsem):
    writer = Writer(spots, out, stage, wsem)
    whole = {"ac": (wac, 0, 512), "bd": (wbd, 0, 512), "e": (wef, 0, 256), "f": (wef, 256, 512), "a": (wac, 0, 256)}
    whole |= {"c": (wac, 256, 512), "b": (wbd, 0, 256), "d": (wbd, 256, 512)}
    for n, (k, l) in enumerate(KEPT):
        writer.emit(k, l, keep[slot(n)])
    m = AT_REST
    for left, rights in REST:
        ref, lo, hi = whole[left.lower()]
        turned[...] = ref[:, lo:hi].T
        for name, cols in rights:
            ref, lo, hi = whole[name]
            result = jnp.dot(turned[...], ref[:, lo:hi], preferred_element_type=jnp.float32)
            for i, k in enumerate(PAIRS[left]):
                for j, l in enumerate(cols):
                    writer.emit(k, l, sall[slot(m)].astype(jnp.float32) - piece(result, i, j))
                    m += 1
    writer.finish()


def border_kernel(spots, yea, yeb, fyea, fyeb, before, out, stage, wsem):
    del before
    writer = Writer(spots, out, stage, wsem)
    for n, (k, l) in enumerate(Y_HIGH):
        writer.emit(k, l, yea[slot(n)] + fyea[slot(n)])
    for n, (k, l) in enumerate(Y_LOW):
        writer.emit(k, l, yeb[slot(n)] + known("gy", fyeb[slot(n)]))
    writer.finish()


def last_kernel(spots, za, zb, fza, fzb, xa, xb, fxa, fxb, before, out, stage, wsem):
    del before
    writer = Writer(spots, out, stage, wsem)
    for pairs, packs, own, other, take in (
        (Z_LOW, Z_LOW_PACK, zb, fzb, lambda value: known("gz", value)),
        (Z_HIGH, Z_HIGH_PACK, za, fza, lambda value: value),
    ):
        for n, (k, l) in enumerate(pairs):
            writer.emit(k, l, own[slot(n)] + take(other[slot(n)]))
        for n, (k, l) in enumerate(packs):
            row = slice(FACES + n, FACES + n + 1)
            first, second = unpack(own[slot(6 + n)] + take(other[slot(6 + n)]), own[row] + take(other[row]))
            writer.emit(k, k, first)
            writer.emit(l, l, second)
    writer.emit(0, 0, xb[...] + known("gx", fxb[...]))
    writer.emit(1, 1, xa[...] + fxa[...])
    writer.finish()


def exchange_high(value, axis):
    return lax.ppermute(value, axis, [(i, i ^ 1) for i in range(lax.axis_size(axis))])


def exchange_low(value, axis):
    size, across = lax.axis_size(axis), lax.axis_size("gx")
    if axis == "gx":
        return lax.ppermute(value, axis, [(i, size - 1 - i) for i in range(size)])
    pairs = []
    for x in range(across):
        for i in range(size):
            to = (x ^ 1, i) if i in (0, size - 1) else (x, ((i - 1) ^ 1) + 1)
            pairs.append((x * size + i, to[0] * size + to[1]))
    return lax.ppermute(value, ("gx", axis), pairs)


def known(axis, value):
    at = lax.axis_index(axis)
    return jnp.where((at > 0) & (at < lax.axis_size(axis) - 1), value, 0.0)


HBM = pl.BlockSpec(memory_space=pltpu.HBM)
VMEM = pl.BlockSpec(memory_space=pltpu.VMEM)
DMA = pltpu.SemaphoreType.DMA


def shape(*dims, dtype=jnp.float32):
    return jax.ShapeDtypeStruct(dims, dtype)


def params(mib):
    return pltpu.CompilerParams(vmem_limit_bytes=mib * 1024 * 1024)


def cost(gigaflops, megabytes):
    return pl.CostEstimate(
        flops=int(gigaflops * 1e9), bytes_accessed=int(megabytes * 1e6), transcendentals=0
    )


def in_hbm(value):
    return pltpu.with_memory_space_constraint(value, pltpu.HBM)


def shards(inv_factor, coupling, stiff_gg, block_order):
    rows = inv_factor.shape[3]
    size = NBLK * BLK
    half = jnp.bfloat16
    order = in_hbm(block_order.reshape(NBLK))
    inverse = in_hbm(inv_factor.reshape(rows, rows))
    coupled = in_hbm(coupling.reshape(rows, size))
    stiff = in_hbm(stiff_gg.reshape(size, size))
    panels = rows // PAN
    osmem = pltpu.SMEM((NBLK,), jnp.int32)

    lbuf, cbuf, sall, wbd, yda, ydb, zpart, spots = pl.pallas_call(
        edge_kernel,
        out_shape=(
            shape(rows, rows, dtype=half),
            shape(rows, size, dtype=half),
            shape(len(LATER) * BLK, BLK, dtype=half),
            shape(rows, 512, dtype=half),
            shape(BLK + 8, BLK),
            shape(BLK + 8, BLK),
            shape(4 * BLK + 8, BLK),
            shape(8, BLK, dtype=jnp.int32),
        ),
        in_specs=[HBM] * 4,
        out_specs=(VMEM,) * 8,
        scratch_shapes=[osmem, pltpu.VMEM((len(EDGE_BLOCKS) * BLK, BLK), half), DMA, DMA((panels,)), DMA((panels,)), DMA, DMA],
        compiler_params=params(12),
        cost_estimate=cost(3, 8),
        name="edges",
    )(order, inverse, coupled, stiff)
    fya = exchange_high(yda, "gy")
    fyb = exchange_low(ydb, "gy")
    wac, za, zb = pl.pallas_call(
        face_kernel,
        out_shape=(shape(rows, 512, dtype=half), shape(MESSAGE, BLK), shape(MESSAGE, BLK)),
        in_specs=[VMEM] * 5,
        out_specs=(VMEM,) * 3,
        compiler_params=params(12),
        cost_estimate=cost(3, 1),
        name="faces",
    )(sall, lbuf, cbuf, wbd, zpart)
    za, zb = pl.pallas_call(
        join_kernel,
        out_shape=(shape(MESSAGE, BLK), shape(MESSAGE, BLK)),
        in_specs=[VMEM] * 4,
        out_specs=(VMEM,) * 2,
        input_output_aliases={0: 0, 1: 1},
        compiler_params=params(2),
        cost_estimate=cost(0.1, 0.1),
        name="join",
    )(za, zb, fya, fyb)
    fzb = exchange_low(zb, "gz")
    fza = exchange_high(za, "gz")
    wef, yea, yeb, xa, xb, keep = pl.pallas_call(
        side_kernel,
        out_shape=(
            shape(rows, 512, dtype=half),
            shape(4 * BLK, BLK),
            shape(4 * BLK, BLK),
            shape(BLK, BLK),
            shape(BLK, BLK),
            shape(len(KEPT) * BLK, BLK),
        ),
        in_specs=[VMEM] * 5,
        out_specs=(VMEM,) * 6,
        compiler_params=params(12),
        cost_estimate=cost(3, 1),
        name="sides",
    )(sall, lbuf, cbuf, wbd, za)
    fyea = exchange_high(yea, "gy")
    fyeb = exchange_low(yeb, "gy")
    fxa = exchange_high(xa, "gx")
    fxb = exchange_low(xb, "gx")
    out = pl.pallas_call(
        rest_kernel,
        out_shape=shape(size, size),
        in_specs=[VMEM] * 6,
        out_specs=HBM,
        scratch_shapes=[
            pltpu.VMEM((PAN, rows), half),
            pltpu.VMEM((2 * (len(KEPT) + len(REST_BLOCKS)) * BLK, BLK), jnp.float32),
            DMA,
        ],
        compiler_params=params(16),
        cost_estimate=cost(3, 8),
        name="rest",
    )(spots, sall, wbd, wac, wef, keep)
    out = pl.pallas_call(
        border_kernel,
        out_shape=shape(size, size),
        in_specs=[VMEM] * 5 + [HBM],
        out_specs=HBM,
        scratch_shapes=[pltpu.VMEM((14 * BLK, BLK), jnp.float32), DMA],
        input_output_aliases={5: 0},
        compiler_params=params(4),
        cost_estimate=cost(0.1, 1),
        name="borders",
    )(spots, yea, yeb, fyea, fyeb, out)
    out = pl.pallas_call(
        last_kernel,
        out_shape=shape(size, size),
        in_specs=[VMEM] * 9 + [HBM],
        out_specs=HBM,
        scratch_shapes=[pltpu.VMEM((34 * BLK, BLK), jnp.float32), DMA],
        input_output_aliases={9: 0},
        compiler_params=params(8),
        cost_estimate=cost(0.1, 2),
        name="last",
    )(spots, za, zb, fza, fzb, xa, xb, fxa, fxb, out)
    return out.reshape(1, 1, 1, size, size)


def solution(mesh):
    return jax.shard_map(
        shards,
        mesh=mesh,
        in_specs=(
            P("gx", "gy", "gz", None, None),
            P("gx", "gy", "gz", None, None),
            P("gx", "gy", "gz", None, None),
            P("gx", "gy", "gz", None),
        ),
        out_specs=P("gx", "gy", "gz", None, None),
        check_vma=False,
    )
```

```python
import jax
import jax.numpy as jnp
from jax import lax
from jax.experimental import pallas as pl
from jax.experimental.pallas import tpu as pltpu
from jax.sharding import PartitionSpec as P


BLK = 128
NBLK = 12
PAN = 256

PAIRS = {"A": (4, 5), "B": (8, 9), "C": (6, 7), "D": (10, 11), "E": (2, 3), "F": (0, 1)}
COLUMNS = (8, 9, 10, 11, 4, 5, 6, 7, 2, 3, 0, 1)
Z_HIGH, Z_LOW = ((6, 7), (6, 10), (6, 11), (7, 10), (7, 11), (10, 11)), ((4, 5), (4, 8), (4, 9), (5, 8), (5, 9), (8, 9))
Z_HIGH_PACK, Z_LOW_PACK = ((6, 7), (11, 10)), ((4, 5), (8, 9))
Y_HIGH, Y_LOW = ((3, 3), (3, 9), (3, 11), (9, 11)), ((2, 2), (2, 8), (2, 10), (8, 10))
KEPT = ((2, 3), (2, 9), (3, 8), (2, 11), (3, 10), (8, 11), (9, 10), (0, 1))
FACES = 8 * BLK
GROUPS = ((0, 2), (2, 4), (4, 6))
MESSAGE = FACES + 8


def position(order, k):
    if k < 2:
        at = k ^ (lax.axis_index("gx") % 2)
    elif k < 4:
        at = 2 + ((k - 2) ^ (lax.axis_index("gy") % 2))
    elif k < 8:
        at = 4 + ((k - 4) ^ (2 * (lax.axis_index("gz") % 2)))
    else:
        at = 8 + ((k - 8) ^ (lax.axis_index("gy") % 2 + 2 * (lax.axis_index("gz") % 2)))
    return pl.multiple_of(order[at] * BLK, BLK)


def positions(order):
    return [position(order, k) for k in range(NBLK)]


def fetch_order(order, osmem, sem):
    copy = pltpu.make_async_copy(order, osmem, sem)
    copy.start()
    return copy


def stiff_copies(at, stiff, buf, sem, blocks):
    return [
        pltpu.make_async_copy(
            stiff.at[pl.ds(at[k], BLK), pl.ds(at[l], BLK)], buf.at[pl.ds(n * BLK, BLK), :], sem
        )
        for n, (k, l) in enumerate(blocks)
    ]


def weigh(lbuf, cbuf, columns, pan):
    depth = (pan + 1) * PAN
    return jnp.dot(
        lbuf[pan * PAN : depth, :depth], cbuf[:depth, columns], preferred_element_type=jnp.float32
    ).astype(jnp.bfloat16)


def gram(left, right):
    return lax.dot_general(left, right, (((0,), (0,)), ((), ())), preferred_element_type=jnp.float32)


def rows_ge():
    r = lax.broadcasted_iota(jnp.int32, (BLK, BLK), 0)
    c = lax.broadcasted_iota(jnp.int32, (BLK, BLK), 1)
    return r, c


def pack(first, second):
    r, c = rows_ge()
    return jnp.where(r <= c, first, second), jnp.sum(jnp.where(r == c, second, 0.0), axis=0, keepdims=True)


def unpack(tile, diagonal):
    r, c = rows_ge()
    turned = tile.T
    first = jnp.where(r <= c, tile, turned)
    return first, jnp.where(r > c, tile, jnp.where(r < c, turned, diagonal))


def two_rows(first, second):
    row = lax.broadcasted_iota(jnp.int32, (8, BLK), 0)
    return jnp.where(row == 0, first, jnp.where(row == 1, second, 0.0))


def piece(result, i, j):
    return result[i * BLK : (i + 1) * BLK, j * BLK : (j + 1) * BLK]


def slot(n):
    return slice(n * BLK, (n + 1) * BLK)


FACE_BLOCKS = ((4, 4), (4, 5), (5, 5), (4, 8), (4, 9), (5, 8), (5, 9), (6, 6), (6, 7), (7, 7), (6, 10), (6, 11), (7, 10), (7, 11))
SIDE_BLOCKS = tuple((k, l) for k in (2, 3) for l in (2, 3, 8, 9, 10, 11) if k <= l) + ((8, 10), (8, 11), (9, 10), (9, 11), (0, 0), (0, 1), (1, 1))
REST = (
    ("F", (("bd", (8, 9, 10, 11)), ("ac", (4, 5, 6, 7)), ("e", (2, 3)))),
    ("E", (("ac", (4, 5, 6, 7)),)),
    ("A", (("c", (6, 7)), ("d", (10, 11)))),
    ("C", (("b", (8, 9)),)),
)
REST_BLOCKS = tuple((k, l) for left, rights in REST for _, cols in rights for k in PAIRS[left] for l in cols)
LATER = FACE_BLOCKS + SIDE_BLOCKS + REST_BLOCKS
AT_FACES, AT_SIDES, AT_REST = 0, len(FACE_BLOCKS), len(FACE_BLOCKS) + len(SIDE_BLOCKS)
EDGE_BLOCKS = ((8, 8), (8, 9), (9, 9), (10, 10), (10, 11), (11, 11))


def edge_kernel(order, inverse, coupling, stiff, lbuf, cbuf, sall, wbd, yda, ydb, zpart, spots, osmem, sbuf, osem, lsem, csem, rsem, ssem):
    fetch = fetch_order(order, osmem, osem)
    panels = lbuf.shape[0] // PAN
    lcopies = [
        pltpu.make_async_copy(
            inverse.at[pl.ds(pan * PAN, PAN), pl.ds(0, (pan + 1) * PAN)],
            lbuf.at[pl.ds(pan * PAN, PAN), pl.ds(0, (pan + 1) * PAN)],
            lsem.at[pan],
        )
        for pan in range(panels)
    ]
    for copy in lcopies:
        copy.start()
    fetch.wait()
    at = positions(osmem)
    lane = lax.broadcasted_iota(jnp.int32, (8, BLK), 1)
    spots[...] = sum(jnp.where(lane == k, at[k], 0) for k in range(NBLK))
    ccopies = []
    for lo, hi in GROUPS:
        rows = pl.ds(lo * PAN, (hi - lo) * PAN)
        group = [
            pltpu.make_async_copy(
                coupling.at[rows, pl.ds(at[k], BLK)], cbuf.at[rows, pl.ds(n * BLK, BLK)], csem.at[lo]
            )
            for n, k in enumerate(COLUMNS[:4])
        ]
        ccopies.append(group)
        for copy in group:
            copy.start()
    scopies = stiff_copies(at, stiff, sbuf, ssem, EDGE_BLOCKS)
    for copy in scopies:
        copy.start()
    later = [
        pltpu.make_async_copy(
            coupling.at[:, pl.ds(at[k], BLK)], cbuf.at[:, pl.ds((n + 4) * BLK, BLK)], rsem
        )
        for n, k in enumerate(COLUMNS[4:])
    ]
    later += stiff_copies(at, stiff, sall, rsem, LATER)
    for (lo, hi), group in zip(GROUPS, ccopies):
        for pan in range(lo, hi):
            lcopies[pan].wait()
        for copy in group:
            copy.wait()
        if lo == 0:
            for copy in later:
                copy.start()
        for pan in range(lo, hi):
            wbd[pan * PAN : (pan + 1) * PAN, :] = weigh(lbuf, cbuf, slice(0, 512), pan)
    for copy in scopies:
        copy.wait()
    full = []
    for n in range(2):
        half = wbd[:, n * 256 : (n + 1) * 256]
        result = gram(half, half)
        for m, (i, j) in enumerate(((0, 0), (0, 1), (1, 1))):
            full.append(sbuf[slot(n * 3 + m)].astype(jnp.float32) - piece(result, i, j))
    b8, b89, b9, b10, b1011, b11 = full
    ydb[:BLK], row = pack(b8, b10)
    ydb[BLK:] = two_rows(row, 0.0)
    yda[:BLK], row = pack(b11, b9)
    yda[BLK:] = two_rows(row, 0.0)
    zpart[slot(0)] = b89
    zpart[slot(1)] = b1011
    zpart[slot(2)], low = pack(b8, b9)
    zpart[slot(3)], high = pack(b11, b10)
    zpart[4 * BLK :] = two_rows(low, high)
    for copy in later:
        copy.wait()


def face_kernel(sall, lbuf, cbuf, wbd, zpart, wac, za, zb):
    for pan in range(lbuf.shape[0] // PAN):
        wac[pan * PAN : (pan + 1) * PAN, :] = weigh(lbuf, cbuf, slice(512, 1024), pan)
    for n, (out, part) in enumerate(((zb, 0), (za, 1))):
        own = wac[:, n * 256 : (n + 1) * 256]
        inner = gram(own, own)
        outer = gram(own, wbd[:, n * 256 : (n + 1) * 256])
        base = AT_FACES + n * 7

        def value(m, result, i, j):
            return sall[slot(base + m)].astype(jnp.float32) - piece(result, i, j)

        out[slot(6)], row = pack(value(0, inner, 0, 0), value(2, inner, 1, 1))
        out[slot(0)] = value(1, inner, 0, 1)
        for m, (i, j) in enumerate(((0, 0), (0, 1), (1, 0), (1, 1))):
            out[slot(1 + m)] = value(3 + m, outer, i, j)
        out[slot(5)] = zpart[slot(part)]
        out[slot(7)] = zpart[slot(2 + part)]
        out[FACES:] = two_rows(row, zpart[4 * BLK + part : 4 * BLK + part + 1])


def join_kernel(za, zb, fya, fyb, za_out, zb_out):
    del za, zb
    r, c = rows_ge()
    above = r <= c
    row = lax.broadcasted_iota(jnp.int32, (8, BLK), 0) == 1
    below, diagonal = known("gy", fyb[:BLK]), known("gy", fyb[BLK : BLK + 1])
    za_out[slot(7)] = za_out[slot(7)] + jnp.where(above, fya[:BLK], below)
    za_out[FACES:] = za_out[FACES:] + jnp.where(row, diagonal, 0.0)
    zb_out[slot(7)] = zb_out[slot(7)] + jnp.where(above, below, fya[:BLK])
    zb_out[FACES:] = zb_out[FACES:] + jnp.where(row, fya[BLK : BLK + 1], 0.0)


def side_kernel(sall, lbuf, cbuf, wbd, after, wef, yea, yeb, xa, xb, keep):
    del after
    for pan in range(lbuf.shape[0] // PAN):
        wef[pan * PAN : (pan + 1) * PAN, :] = weigh(lbuf, cbuf, slice(1024, 1536), pan)
    e, f = wef[:, :256], wef[:, 256:]
    targets = {pair: (yea, n) for n, pair in enumerate(Y_HIGH)} | {pair: (yeb, n) for n, pair in enumerate(Y_LOW)}
    targets |= {pair: (keep, n) for n, pair in enumerate(KEPT)} | {(1, 1): (xa, 0), (0, 0): (xb, 0)}

    def emit(result, rows, cols):
        for i, k in enumerate(rows):
            for j, l in enumerate(cols):
                if k <= l:
                    out, n = targets[(k, l)]
                    m = AT_SIDES + SIDE_BLOCKS.index((k, l))
                    out[slot(n)] = sall[slot(m)].astype(jnp.float32) - piece(result, i, j)

    emit(gram(e, e), (2, 3), (2, 3))
    emit(gram(e, wbd[...]), (2, 3), (8, 9, 10, 11))
    emit(gram(wbd[:, :256], wbd[:, 256:]), (8, 9), (10, 11))
    emit(gram(f, f), (0, 1), (0, 1))


class Writer:
    def __init__(self, spots, out, stage, sem):
        row = spots[0:1, :]
        self.at = [pl.multiple_of(row[0, k], BLK) for k in range(NBLK)]
        self.out, self.stage, self.sem, self.copies = out, stage, sem, []

    def put(self, k, l, value):
        n = len(self.copies)
        self.stage[slot(n)] = value
        copy = pltpu.make_async_copy(
            self.stage.at[pl.ds(n * BLK, BLK), :],
            self.out.at[pl.ds(self.at[k], BLK), pl.ds(self.at[l], BLK)],
            self.sem,
        )
        copy.start()
        self.copies.append(copy)

    def emit(self, k, l, value):
        self.put(k, l, value)
        if k != l:
            self.put(l, k, value.T)

    def finish(self):
        for copy in self.copies:
            copy.wait()


def rest_kernel(spots, sall, wbd, wac, wef, keep, out, turned, stage, wsem):
    writer = Writer(spots, out, stage, wsem)
    whole = {"ac": (wac, 0, 512), "bd": (wbd, 0, 512), "e": (wef, 0, 256), "f": (wef, 256, 512), "a": (wac, 0, 256)}
    whole |= {"c": (wac, 256, 512), "b": (wbd, 0, 256), "d": (wbd, 256, 512)}
    for n, (k, l) in enumerate(KEPT):
        writer.emit(k, l, keep[slot(n)])
    m = AT_REST
    for left, rights in REST:
        ref, lo, hi = whole[left.lower()]
        turned[...] = ref[:, lo:hi].T
        for name, cols in rights:
            ref, lo, hi = whole[name]
            result = jnp.dot(turned[...], ref[:, lo:hi], preferred_element_type=jnp.float32)
            for i, k in enumerate(PAIRS[left]):
                for j, l in enumerate(cols):
                    writer.emit(k, l, sall[slot(m)].astype(jnp.float32) - piece(result, i, j))
                    m += 1
    writer.finish()


def border_kernel(spots, yea, yeb, fyea, fyeb, xa, fxa, before, out, stage, wsem):
    del before
    writer = Writer(spots, out, stage, wsem)
    for n, (k, l) in enumerate(Y_HIGH):
        writer.emit(k, l, yea[slot(n)] + fyea[slot(n)])
    for n, (k, l) in enumerate(Y_LOW):
        writer.emit(k, l, yeb[slot(n)] + known("gy", fyeb[slot(n)]))
    writer.emit(1, 1, xa[...] + fxa[...])
    writer.finish()


def last_kernel(spots, za, zb, fza, fzb, before, out, stage, wsem):
    del before
    writer = Writer(spots, out, stage, wsem)
    for pairs, packs, own, other, take in (
        (Z_LOW, Z_LOW_PACK, zb, fzb, lambda value: known("gz", value)),
        (Z_HIGH, Z_HIGH_PACK, za, fza, lambda value: value),
    ):
        for n, (k, l) in enumerate(pairs):
            writer.emit(k, l, own[slot(n)] + take(other[slot(n)]))
        for n, (k, l) in enumerate(packs):
            row = slice(FACES + n, FACES + n + 1)
            first, second = unpack(own[slot(6 + n)] + take(other[slot(6 + n)]), own[row] + take(other[row]))
            writer.emit(k, k, first)
            writer.emit(l, l, second)
    writer.finish()


def corner_kernel(spots, xb, fxb, before, out, stage, wsem):
    del before
    writer = Writer(spots, out, stage, wsem)
    writer.emit(0, 0, xb[...] + known("gx", fxb[...]))
    writer.finish()


def exchange_high(value, axis):
    return lax.ppermute(value, axis, [(i, i ^ 1) for i in range(lax.axis_size(axis))])


def exchange_low(value, axis):
    size, across = lax.axis_size(axis), lax.axis_size("gx")
    if axis == "gx":
        rows = lax.axis_size("gy")
        pairs = []
        for i in range(size):
            for y in range(rows):
                to = (i, y ^ 1) if i in (0, size - 1) else (size - 1 - i, y)
                pairs.append((i * rows + y, to[0] * rows + to[1]))
        return lax.ppermute(value, ("gx", "gy"), pairs)
    pairs = []
    for x in range(across):
        for i in range(size):
            to = (x ^ 1, i) if i in (0, size - 1) else (x, ((i - 1) ^ 1) + 1)
            pairs.append((x * size + i, to[0] * size + to[1]))
    return lax.ppermute(value, ("gx", axis), pairs)


def known(axis, value):
    at = lax.axis_index(axis)
    return jnp.where((at > 0) & (at < lax.axis_size(axis) - 1), value, 0.0)


HBM = pl.BlockSpec(memory_space=pltpu.HBM)
VMEM = pl.BlockSpec(memory_space=pltpu.VMEM)
DMA = pltpu.SemaphoreType.DMA


def shape(*dims, dtype=jnp.float32):
    return jax.ShapeDtypeStruct(dims, dtype)


def params(mib):
    return pltpu.CompilerParams(vmem_limit_bytes=mib * 1024 * 1024)


def cost(gigaflops, megabytes):
    return pl.CostEstimate(
        flops=int(gigaflops * 1e9), bytes_accessed=int(megabytes * 1e6), transcendentals=0
    )


def in_hbm(value):
    return pltpu.with_memory_space_constraint(value, pltpu.HBM)


def shards(inv_factor, coupling, stiff_gg, block_order):
    rows = inv_factor.shape[3]
    size = NBLK * BLK
    half = jnp.bfloat16
    order = in_hbm(block_order.reshape(NBLK))
    inverse = in_hbm(inv_factor.reshape(rows, rows))
    coupled = in_hbm(coupling.reshape(rows, size))
    stiff = in_hbm(stiff_gg.reshape(size, size))
    panels = rows // PAN
    osmem = pltpu.SMEM((NBLK,), jnp.int32)

    lbuf, cbuf, sall, wbd, yda, ydb, zpart, spots = pl.pallas_call(
        edge_kernel,
        out_shape=(
            shape(rows, rows, dtype=half),
            shape(rows, size, dtype=half),
            shape(len(LATER) * BLK, BLK, dtype=half),
            shape(rows, 512, dtype=half),
            shape(BLK + 8, BLK),
            shape(BLK + 8, BLK),
            shape(4 * BLK + 8, BLK),
            shape(8, BLK, dtype=jnp.int32),
        ),
        in_specs=[HBM] * 4,
        out_specs=(VMEM,) * 8,
        scratch_shapes=[osmem, pltpu.VMEM((len(EDGE_BLOCKS) * BLK, BLK), half), DMA, DMA((panels,)), DMA((panels,)), DMA, DMA],
        compiler_params=params(12),
        cost_estimate=cost(3, 8),
        name="edges",
    )(order, inverse, coupled, stiff)
    fya = exchange_high(yda, "gy")
    fyb = exchange_low(ydb, "gy")
    wac, za, zb = pl.pallas_call(
        face_kernel,
        out_shape=(shape(rows, 512, dtype=half), shape(MESSAGE, BLK), shape(MESSAGE, BLK)),
        in_specs=[VMEM] * 5,
        out_specs=(VMEM,) * 3,
        compiler_params=params(12),
        cost_estimate=cost(3, 1),
        name="faces",
    )(sall, lbuf, cbuf, wbd, zpart)
    za, zb = pl.pallas_call(
        join_kernel,
        out_shape=(shape(MESSAGE, BLK), shape(MESSAGE, BLK)),
        in_specs=[VMEM] * 4,
        out_specs=(VMEM,) * 2,
        input_output_aliases={0: 0, 1: 1},
        compiler_params=params(2),
        cost_estimate=cost(0.1, 0.1),
        name="join",
    )(za, zb, fya, fyb)
    fzb = exchange_low(zb, "gz")
    fza = exchange_high(za, "gz")
    wef, yea, yeb, xa, xb, keep = pl.pallas_call(
        side_kernel,
        out_shape=(
            shape(rows, 512, dtype=half),
            shape(4 * BLK, BLK),
            shape(4 * BLK, BLK),
            shape(BLK, BLK),
            shape(BLK, BLK),
            shape(len(KEPT) * BLK, BLK),
        ),
        in_specs=[VMEM] * 5,
        out_specs=(VMEM,) * 6,
        compiler_params=params(12),
        cost_estimate=cost(3, 1),
        name="sides",
    )(sall, lbuf, cbuf, wbd, za)
    fyea = exchange_high(yea, "gy")
    fyeb = exchange_low(yeb, "gy")
    fxa = exchange_high(xa, "gx")
    fxb = exchange_low(xb, "gx")
    out = pl.pallas_call(
        rest_kernel,
        out_shape=shape(size, size),
        in_specs=[VMEM] * 6,
        out_specs=HBM,
        scratch_shapes=[
            pltpu.VMEM((PAN, rows), half),
            pltpu.VMEM((2 * (len(KEPT) + len(REST_BLOCKS)) * BLK, BLK), jnp.float32),
            DMA,
        ],
        compiler_params=params(16),
        cost_estimate=cost(3, 8),
        name="rest",
    )(spots, sall, wbd, wac, wef, keep)
    out = pl.pallas_call(
        border_kernel,
        out_shape=shape(size, size),
        in_specs=[VMEM] * 7 + [HBM],
        out_specs=HBM,
        scratch_shapes=[pltpu.VMEM((15 * BLK, BLK), jnp.float32), DMA],
        input_output_aliases={7: 0},
        compiler_params=params(4),
        cost_estimate=cost(0.1, 1),
        name="borders",
    )(spots, yea, yeb, fyea, fyeb, xa, fxa, out)
    out = pl.pallas_call(
        last_kernel,
        out_shape=shape(size, size),
        in_specs=[VMEM] * 5 + [HBM],
        out_specs=HBM,
        scratch_shapes=[pltpu.VMEM((32 * BLK, BLK), jnp.float32), DMA],
        input_output_aliases={5: 0},
        compiler_params=params(8),
        cost_estimate=cost(0.1, 2),
        name="last",
    )(spots, za, zb, fza, fzb, out)
    out = pl.pallas_call(
        corner_kernel,
        out_shape=shape(size, size),
        in_specs=[VMEM] * 3 + [HBM],
        out_specs=HBM,
        scratch_shapes=[pltpu.VMEM((BLK, BLK), jnp.float32), DMA],
        input_output_aliases={3: 0},
        compiler_params=params(2),
        cost_estimate=cost(0.01, 0.1),
        name="end",
    )(spots, xb, fxb, out)
    return out.reshape(1, 1, 1, size, size)


def solution(mesh):
    return jax.shard_map(
        shards,
        mesh=mesh,
        in_specs=(
            P("gx", "gy", "gz", None, None),
            P("gx", "gy", "gz", None, None),
            P("gx", "gy", "gz", None, None),
            P("gx", "gy", "gz", None),
        ),
        out_specs=P("gx", "gy", "gz", None, None),
        check_vma=False,
    )
```

```python
import jax
import jax.numpy as jnp
from jax import lax
from jax.experimental import pallas as pl
from jax.experimental.pallas import tpu as pltpu
from jax.sharding import PartitionSpec as P


BLK = 128
NBLK = 12
PAN = 256

PAIRS = {"A": (4, 5), "B": (8, 9), "C": (6, 7), "D": (10, 11), "E": (2, 3), "F": (0, 1)}
COLUMNS = (8, 9, 10, 11, 4, 5, 6, 7, 2, 3, 0, 1)
Z_HIGH, Z_LOW = ((6, 7), (6, 10), (6, 11), (7, 10), (7, 11), (10, 11)), ((4, 5), (4, 8), (4, 9), (5, 8), (5, 9), (8, 9))
Z_HIGH_PACK, Z_LOW_PACK = ((6, 7), (11, 10)), ((4, 5), (8, 9))
Y_HIGH, Y_LOW = ((3, 3), (3, 9), (3, 11), (9, 11)), ((2, 2), (2, 8), (2, 10), (8, 10))
KEPT = ((2, 3), (2, 9), (3, 8), (2, 11), (3, 10), (8, 11), (9, 10), (0, 1))
FACES = 8 * BLK
GROUPS = ((0, 1), (1, 3), (3, 6))
HEAD = GROUPS[0][1] * PAN
MESSAGE = FACES + 8


def position(order, k):
    if k < 2:
        at = k ^ (lax.axis_index("gx") % 2)
    elif k < 4:
        at = 2 + ((k - 2) ^ (lax.axis_index("gy") % 2))
    elif k < 8:
        at = 4 + ((k - 4) ^ (2 * (lax.axis_index("gz") % 2)))
    else:
        at = 8 + ((k - 8) ^ (lax.axis_index("gy") % 2 + 2 * (lax.axis_index("gz") % 2)))
    return pl.multiple_of(order[at] * BLK, BLK)


def positions(order):
    return [position(order, k) for k in range(NBLK)]


def fetch_order(order, osmem, sem):
    copy = pltpu.make_async_copy(order, osmem, sem)
    copy.start()
    return copy


def stiff_copies(at, stiff, buf, sem, blocks):
    return [
        pltpu.make_async_copy(
            stiff.at[pl.ds(at[k], BLK), pl.ds(at[l], BLK)], buf.at[pl.ds(n * BLK, BLK), :], sem
        )
        for n, (k, l) in enumerate(blocks)
    ]


def weigh(lbuf, cbuf, columns, pan):
    depth = (pan + 1) * PAN
    return jnp.dot(
        lbuf[pan * PAN : depth, :depth], cbuf[:depth, columns], preferred_element_type=jnp.float32
    ).astype(jnp.bfloat16)


def gram(left, right):
    return lax.dot_general(left, right, (((0,), (0,)), ((), ())), preferred_element_type=jnp.float32)


def rows_ge():
    r = lax.broadcasted_iota(jnp.int32, (BLK, BLK), 0)
    c = lax.broadcasted_iota(jnp.int32, (BLK, BLK), 1)
    return r, c


def pack(first, second):
    r, c = rows_ge()
    return jnp.where(r <= c, first, second), jnp.sum(jnp.where(r == c, second, 0.0), axis=0, keepdims=True)


def unpack(tile, diagonal):
    r, c = rows_ge()
    turned = tile.T
    first = jnp.where(r <= c, tile, turned)
    return first, jnp.where(r > c, tile, jnp.where(r < c, turned, diagonal))


def two_rows(first, second):
    row = lax.broadcasted_iota(jnp.int32, (8, BLK), 0)
    return jnp.where(row == 0, first, jnp.where(row == 1, second, 0.0))


def piece(result, i, j):
    return result[i * BLK : (i + 1) * BLK, j * BLK : (j + 1) * BLK]


def slot(n):
    return slice(n * BLK, (n + 1) * BLK)


FACE_BLOCKS = ((4, 4), (4, 5), (5, 5), (4, 8), (4, 9), (5, 8), (5, 9), (6, 6), (6, 7), (7, 7), (6, 10), (6, 11), (7, 10), (7, 11))
SIDE_BLOCKS = tuple((k, l) for k in (2, 3) for l in (2, 3, 8, 9, 10, 11) if k <= l) + ((8, 10), (8, 11), (9, 10), (9, 11), (0, 0), (0, 1), (1, 1))
REST = (
    ("F", (("bd", (8, 9, 10, 11)), ("ac", (4, 5, 6, 7)), ("e", (2, 3)))),
    ("E", (("ac", (4, 5, 6, 7)),)),
    ("A", (("c", (6, 7)), ("d", (10, 11)))),
    ("C", (("b", (8, 9)),)),
)
REST_BLOCKS = tuple((k, l) for left, rights in REST for _, cols in rights for k in PAIRS[left] for l in cols)
LATER = FACE_BLOCKS + SIDE_BLOCKS + REST_BLOCKS
AT_FACES, AT_SIDES, AT_REST = 0, len(FACE_BLOCKS), len(FACE_BLOCKS) + len(SIDE_BLOCKS)
EDGE_BLOCKS = ((8, 8), (8, 9), (9, 9), (10, 10), (10, 11), (11, 11))


def edge_kernel(order, inverse, coupling, stiff, lbuf, cbuf, sall, wbd, yda, ydb, zpart, spots, osmem, sbuf, crow, osem, hsem, lsem, csem, rsem, ssem):
    fetch = fetch_order(order, osmem, osem)
    panels = lbuf.shape[0] // PAN
    lcopies = [
        pltpu.make_async_copy(
            inverse.at[pl.ds(pan * PAN, PAN), pl.ds(0, (pan + 1) * PAN)],
            lbuf.at[pl.ds(pan * PAN, PAN), pl.ds(0, (pan + 1) * PAN)],
            lsem.at[pan],
        )
        for pan in range(panels)
    ]
    head = pltpu.make_async_copy(coupling.at[pl.ds(0, HEAD), :], crow, hsem)
    for copy in (*lcopies[: GROUPS[0][1]], head, *lcopies[GROUPS[0][1] :]):
        copy.start()
    fetch.wait()
    at = positions(osmem)
    lane = lax.broadcasted_iota(jnp.int32, (8, BLK), 1)
    spots[...] = sum(jnp.where(lane == k, at[k], 0) for k in range(NBLK))
    ccopies = []
    for lo, hi in GROUPS[1:]:
        rows = pl.ds(lo * PAN, (hi - lo) * PAN)
        group = [
            pltpu.make_async_copy(
                coupling.at[rows, pl.ds(at[k], BLK)], cbuf.at[rows, pl.ds(n * BLK, BLK)], csem.at[lo]
            )
            for n, k in enumerate(COLUMNS[:4])
        ]
        ccopies.append(group)
        for copy in group:
            copy.start()
    scopies = stiff_copies(at, stiff, sbuf, ssem, EDGE_BLOCKS)
    for copy in scopies:
        copy.start()
    later = [
        pltpu.make_async_copy(
            coupling.at[:, pl.ds(at[k], BLK)], cbuf.at[:, pl.ds((n + 4) * BLK, BLK)], rsem
        )
        for n, k in enumerate(COLUMNS[4:])
    ]
    later += stiff_copies(at, stiff, sall, rsem, LATER)
    for (lo, hi), group in zip(GROUPS, [[head], *ccopies]):
        for pan in range(lo, hi):
            lcopies[pan].wait()
        for copy in group:
            copy.wait()
        if lo == 0:
            for n, k in enumerate(COLUMNS[:4]):
                cbuf[:HEAD, slot(n)] = crow[:, pl.ds(at[k], BLK)]
        if lo == 0:
            for copy in later:
                copy.start()
        for pan in range(lo, hi):
            wbd[pan * PAN : (pan + 1) * PAN, :] = weigh(lbuf, cbuf, slice(0, 512), pan)
    for copy in scopies:
        copy.wait()
    full = []
    for n in range(2):
        half = wbd[:, n * 256 : (n + 1) * 256]
        result = gram(half, half)
        for m, (i, j) in enumerate(((0, 0), (0, 1), (1, 1))):
            full.append(sbuf[slot(n * 3 + m)].astype(jnp.float32) - piece(result, i, j))
    b8, b89, b9, b10, b1011, b11 = full
    ydb[:BLK], row = pack(b8, b10)
    ydb[BLK:] = two_rows(row, 0.0)
    yda[:BLK], row = pack(b11, b9)
    yda[BLK:] = two_rows(row, 0.0)
    zpart[slot(0)] = b89
    zpart[slot(1)] = b1011
    zpart[slot(2)], low = pack(b8, b9)
    zpart[slot(3)], high = pack(b11, b10)
    zpart[4 * BLK :] = two_rows(low, high)
    for copy in later:
        copy.wait()


def face_kernel(sall, lbuf, cbuf, wbd, zpart, wac, za, zb):
    for pan in range(lbuf.shape[0] // PAN):
        wac[pan * PAN : (pan + 1) * PAN, :] = weigh(lbuf, cbuf, slice(512, 1024), pan)
    for n, (out, part) in enumerate(((zb, 0), (za, 1))):
        own = wac[:, n * 256 : (n + 1) * 256]
        inner = gram(own, own)
        outer = gram(own, wbd[:, n * 256 : (n + 1) * 256])
        base = AT_FACES + n * 7

        def value(m, result, i, j):
            return sall[slot(base + m)].astype(jnp.float32) - piece(result, i, j)

        out[slot(6)], row = pack(value(0, inner, 0, 0), value(2, inner, 1, 1))
        out[slot(0)] = value(1, inner, 0, 1)
        for m, (i, j) in enumerate(((0, 0), (0, 1), (1, 0), (1, 1))):
            out[slot(1 + m)] = value(3 + m, outer, i, j)
        out[slot(5)] = zpart[slot(part)]
        out[slot(7)] = zpart[slot(2 + part)]
        out[FACES:] = two_rows(row, zpart[4 * BLK + part : 4 * BLK + part + 1])


def join_kernel(za, zb, fya, fyb, za_out, zb_out):
    del za, zb
    r, c = rows_ge()
    above = r <= c
    row = lax.broadcasted_iota(jnp.int32, (8, BLK), 0) == 1
    below, diagonal = known("gy", fyb[:BLK]), known("gy", fyb[BLK : BLK + 1])
    za_out[slot(7)] = za_out[slot(7)] + jnp.where(above, fya[:BLK], below)
    za_out[FACES:] = za_out[FACES:] + jnp.where(row, diagonal, 0.0)
    zb_out[slot(7)] = zb_out[slot(7)] + jnp.where(above, below, fya[:BLK])
    zb_out[FACES:] = zb_out[FACES:] + jnp.where(row, fya[BLK : BLK + 1], 0.0)


def side_kernel(sall, lbuf, cbuf, wbd, after, wef, yea, yeb, xa, xb, keep):
    del after
    for pan in range(lbuf.shape[0] // PAN):
        wef[pan * PAN : (pan + 1) * PAN, :] = weigh(lbuf, cbuf, slice(1024, 1536), pan)
    e, f = wef[:, :256], wef[:, 256:]
    targets = {pair: (yea, n) for n, pair in enumerate(Y_HIGH)} | {pair: (yeb, n) for n, pair in enumerate(Y_LOW)}
    targets |= {pair: (keep, n) for n, pair in enumerate(KEPT)} | {(1, 1): (xa, 0), (0, 0): (xb, 0)}

    def emit(result, rows, cols):
        for i, k in enumerate(rows):
            for j, l in enumerate(cols):
                if k <= l:
                    out, n = targets[(k, l)]
                    m = AT_SIDES + SIDE_BLOCKS.index((k, l))
                    out[slot(n)] = sall[slot(m)].astype(jnp.float32) - piece(result, i, j)

    emit(gram(e, e), (2, 3), (2, 3))
    emit(gram(e, wbd[...]), (2, 3), (8, 9, 10, 11))
    emit(gram(wbd[:, :256], wbd[:, 256:]), (8, 9), (10, 11))
    emit(gram(f, f), (0, 1), (0, 1))


class Writer:
    def __init__(self, spots, out, stage, sem):
        row = spots[0:1, :]
        self.at = [pl.multiple_of(row[0, k], BLK) for k in range(NBLK)]
        self.out, self.stage, self.sem, self.copies = out, stage, sem, []

    def put(self, k, l, value):
        n = len(self.copies)
        self.stage[slot(n)] = value
        copy = pltpu.make_async_copy(
            self.stage.at[pl.ds(n * BLK, BLK), :],
            self.out.at[pl.ds(self.at[k], BLK), pl.ds(self.at[l], BLK)],
            self.sem,
        )
        copy.start()
        self.copies.append(copy)

    def emit(self, k, l, value):
        self.put(k, l, value)
        if k != l:
            self.put(l, k, value.T)

    def finish(self):
        for copy in self.copies:
            copy.wait()


def rest_kernel(spots, sall, wbd, wac, wef, keep, out, turned, stage, wsem):
    writer = Writer(spots, out, stage, wsem)
    whole = {"ac": (wac, 0, 512), "bd": (wbd, 0, 512), "e": (wef, 0, 256), "f": (wef, 256, 512), "a": (wac, 0, 256)}
    whole |= {"c": (wac, 256, 512), "b": (wbd, 0, 256), "d": (wbd, 256, 512)}
    for n, (k, l) in enumerate(KEPT):
        writer.emit(k, l, keep[slot(n)])
    m = AT_REST
    for left, rights in REST:
        ref, lo, hi = whole[left.lower()]
        turned[...] = ref[:, lo:hi].T
        for name, cols in rights:
            ref, lo, hi = whole[name]
            result = jnp.dot(turned[...], ref[:, lo:hi], preferred_element_type=jnp.float32)
            for i, k in enumerate(PAIRS[left]):
                for j, l in enumerate(cols):
                    writer.emit(k, l, sall[slot(m)].astype(jnp.float32) - piece(result, i, j))
                    m += 1
    writer.finish()


def border_kernel(spots, yea, yeb, fyea, fyeb, xa, fxa, before, out, stage, wsem):
    del before
    writer = Writer(spots, out, stage, wsem)
    for n, (k, l) in enumerate(Y_HIGH):
        writer.emit(k, l, yea[slot(n)] + fyea[slot(n)])
    for n, (k, l) in enumerate(Y_LOW):
        writer.emit(k, l, yeb[slot(n)] + known("gy", fyeb[slot(n)]))
    writer.emit(1, 1, xa[...] + fxa[...])
    writer.finish()


def last_kernel(spots, za, zb, fza, fzb, before, out, stage, wsem):
    del before
    writer = Writer(spots, out, stage, wsem)
    for pairs, packs, own, other, take in (
        (Z_LOW, Z_LOW_PACK, zb, fzb, lambda value: known("gz", value)),
        (Z_HIGH, Z_HIGH_PACK, za, fza, lambda value: value),
    ):
        for n, (k, l) in enumerate(pairs):
            writer.emit(k, l, own[slot(n)] + take(other[slot(n)]))
        for n, (k, l) in enumerate(packs):
            row = slice(FACES + n, FACES + n + 1)
            first, second = unpack(own[slot(6 + n)] + take(other[slot(6 + n)]), own[row] + take(other[row]))
            writer.emit(k, k, first)
            writer.emit(l, l, second)
    writer.finish()


def corner_kernel(spots, xb, fxb, before, out, stage, wsem):
    del before
    writer = Writer(spots, out, stage, wsem)
    writer.emit(0, 0, xb[...] + known("gx", fxb[...]))
    writer.finish()


def exchange_high(value, axis):
    return lax.ppermute(value, axis, [(i, i ^ 1) for i in range(lax.axis_size(axis))])


def exchange_low(value, axis):
    size, across = lax.axis_size(axis), lax.axis_size("gx")
    if axis == "gx":
        rows = lax.axis_size("gy")
        pairs = []
        for i in range(size):
            for y in range(rows):
                to = (i, y ^ 1) if i in (0, size - 1) else (size - 1 - i, y)
                pairs.append((i * rows + y, to[0] * rows + to[1]))
        return lax.ppermute(value, ("gx", "gy"), pairs)
    pairs = []
    for x in range(across):
        for i in range(size):
            to = (x ^ 1, i) if i in (0, size - 1) else (x, ((i - 1) ^ 1) + 1)
            pairs.append((x * size + i, to[0] * size + to[1]))
    return lax.ppermute(value, ("gx", axis), pairs)


def known(axis, value):
    at = lax.axis_index(axis)
    return jnp.where((at > 0) & (at < lax.axis_size(axis) - 1), value, 0.0)


HBM = pl.BlockSpec(memory_space=pltpu.HBM)
VMEM = pl.BlockSpec(memory_space=pltpu.VMEM)
DMA = pltpu.SemaphoreType.DMA


def shape(*dims, dtype=jnp.float32):
    return jax.ShapeDtypeStruct(dims, dtype)


def params(mib):
    return pltpu.CompilerParams(vmem_limit_bytes=mib * 1024 * 1024)


def cost(gigaflops, megabytes):
    return pl.CostEstimate(
        flops=int(gigaflops * 1e9), bytes_accessed=int(megabytes * 1e6), transcendentals=0
    )


def in_hbm(value):
    return pltpu.with_memory_space_constraint(value, pltpu.HBM)


def shards(inv_factor, coupling, stiff_gg, block_order):
    rows = inv_factor.shape[3]
    size = NBLK * BLK
    half = jnp.bfloat16
    order = in_hbm(block_order.reshape(NBLK))
    inverse = in_hbm(inv_factor.reshape(rows, rows))
    coupled = in_hbm(coupling.reshape(rows, size))
    stiff = in_hbm(stiff_gg.reshape(size, size))
    panels = rows // PAN
    osmem = pltpu.SMEM((NBLK,), jnp.int32)

    lbuf, cbuf, sall, wbd, yda, ydb, zpart, spots = pl.pallas_call(
        edge_kernel,
        out_shape=(
            shape(rows, rows, dtype=half),
            shape(rows, size, dtype=half),
            shape(len(LATER) * BLK, BLK, dtype=half),
            shape(rows, 512, dtype=half),
            shape(BLK + 8, BLK),
            shape(BLK + 8, BLK),
            shape(4 * BLK + 8, BLK),
            shape(8, BLK, dtype=jnp.int32),
        ),
        in_specs=[HBM] * 4,
        out_specs=(VMEM,) * 8,
        scratch_shapes=[osmem, pltpu.VMEM((len(EDGE_BLOCKS) * BLK, BLK), half), pltpu.VMEM((HEAD, size), half), DMA, DMA, DMA((panels,)), DMA((panels,)), DMA, DMA],
        compiler_params=params(12),
        cost_estimate=cost(3, 8),
        name="edges",
    )(order, inverse, coupled, stiff)
    fya = exchange_high(yda, "gy")
    fyb = exchange_low(ydb, "gy")
    wac, za, zb = pl.pallas_call(
        face_kernel,
        out_shape=(shape(rows, 512, dtype=half), shape(MESSAGE, BLK), shape(MESSAGE, BLK)),
        in_specs=[VMEM] * 5,
        out_specs=(VMEM,) * 3,
        compiler_params=params(12),
        cost_estimate=cost(3, 1),
        name="faces",
    )(sall, lbuf, cbuf, wbd, zpart)
    za, zb = pl.pallas_call(
        join_kernel,
        out_shape=(shape(MESSAGE, BLK), shape(MESSAGE, BLK)),
        in_specs=[VMEM] * 4,
        out_specs=(VMEM,) * 2,
        input_output_aliases={0: 0, 1: 1},
        compiler_params=params(2),
        cost_estimate=cost(0.1, 0.1),
        name="join",
    )(za, zb, fya, fyb)
    fzb = exchange_low(zb, "gz")
    fza = exchange_high(za, "gz")
    wef, yea, yeb, xa, xb, keep = pl.pallas_call(
        side_kernel,
        out_shape=(
            shape(rows, 512, dtype=half),
            shape(4 * BLK, BLK),
            shape(4 * BLK, BLK),
            shape(BLK, BLK),
            shape(BLK, BLK),
            shape(len(KEPT) * BLK, BLK),
        ),
        in_specs=[VMEM] * 5,
        out_specs=(VMEM,) * 6,
        compiler_params=params(12),
        cost_estimate=cost(3, 1),
        name="sides",
    )(sall, lbuf, cbuf, wbd, za)
    fyea = exchange_high(yea, "gy")
    fyeb = exchange_low(yeb, "gy")
    fxa = exchange_high(xa, "gx")
    fxb = exchange_low(xb, "gx")
    out = pl.pallas_call(
        rest_kernel,
        out_shape=shape(size, size),
        in_specs=[VMEM] * 6,
        out_specs=HBM,
        scratch_shapes=[
            pltpu.VMEM((PAN, rows), half),
            pltpu.VMEM((2 * (len(KEPT) + len(REST_BLOCKS)) * BLK, BLK), jnp.float32),
            DMA,
        ],
        compiler_params=params(16),
        cost_estimate=cost(3, 8),
        name="rest",
    )(spots, sall, wbd, wac, wef, keep)
    out = pl.pallas_call(
        border_kernel,
        out_shape=shape(size, size),
        in_specs=[VMEM] * 7 + [HBM],
        out_specs=HBM,
        scratch_shapes=[pltpu.VMEM((15 * BLK, BLK), jnp.float32), DMA],
        input_output_aliases={7: 0},
        compiler_params=params(4),
        cost_estimate=cost(0.1, 1),
        name="borders",
    )(spots, yea, yeb, fyea, fyeb, xa, fxa, out)
    out = pl.pallas_call(
        last_kernel,
        out_shape=shape(size, size),
        in_specs=[VMEM] * 5 + [HBM],
        out_specs=HBM,
        scratch_shapes=[pltpu.VMEM((32 * BLK, BLK), jnp.float32), DMA],
        input_output_aliases={5: 0},
        compiler_params=params(8),
        cost_estimate=cost(0.1, 2),
        name="last",
    )(spots, za, zb, fza, fzb, out)
    out = pl.pallas_call(
        corner_kernel,
        out_shape=shape(size, size),
        in_specs=[VMEM] * 3 + [HBM],
        out_specs=HBM,
        scratch_shapes=[pltpu.VMEM((BLK, BLK), jnp.float32), DMA],
        input_output_aliases={3: 0},
        compiler_params=params(2),
        cost_estimate=cost(0.01, 0.1),
        name="end",
    )(spots, xb, fxb, out)
    return out.reshape(1, 1, 1, size, size)


def solution(mesh):
    return jax.shard_map(
        shards,
        mesh=mesh,
        in_specs=(
            P("gx", "gy", "gz", None, None),
            P("gx", "gy", "gz", None, None),
            P("gx", "gy", "gz", None, None),
            P("gx", "gy", "gz", None),
        ),
        out_specs=P("gx", "gy", "gz", None, None),
        check_vma=False,
    )
```
